768 devices in a mesh: dp: 32 (over x, y), seq: 24 (over z, core).
Axes of the slice: x: 4, y: 8, z: 12, core: 2. Of those that a mesh axis runs over, the one named last changes fastest.
Arguments:
- grad_rows: bfloat16 [32, 1920, 4, 1280], P('dp', 'seq'), may hold values from -6 to 6
- row_owner: int32 [32, 1920, 1], P('dp', 'seq'), may hold values from 0 to 23; in each aligned block of 80 rows (0 to 79, 80 to 159, ..., all dimensions but the last counted through in order) at most 4 rows name the same one
- acts: bfloat16 [32, 24, 96, 4, 1280], P('dp', 'seq'), may hold values from -6 to 6
- xact: bfloat16 [32, 24, 96, 4, 1280], P('dp', 'seq'), may hold values from -72 to 72
- gamma: float32 [1280], replicated, may hold values from 0.25 to 1.75
- w_out: bfloat16 [1280, 1280], replicated, may hold values from -0.15625 to 0.15625
Outputs:
- attn_grad: bfloat16 [32, 24, 96, 4, 1280], P('dp', 'seq')
- weight_grad: float32 [1280, 1280], P('dp')
- gain_grad: float32 [1280], replicated
The draws below stay inside these ranges and needn't reach their ends.
Inputs may be any that keep to these rules, and one draw needn't show every extreme that they name: `row_owner`: within the rows of one device (each aligned block of 80 rows) no owner is named more than 4 times, a bound that some block reaches.
All inputs are finite; a program needn't handle non-finite values.
Results may differ from the reference program's by a relative error of at most 0.0049.
Values may be sent and summed in bfloat16 or wider, within the bound.
No kernel may reach another device: no remote copies, remote signals or barrier semaphores. Data moves between devices by JAX's collectives and lax.ppermute only.
A program may use at most 64 MiB of HBM per device.

```python
import math
import jax
import jax.numpy as jnp
import numpy as np
from jax import lax

DV = 1280
PM = 4
TOK_DEV = 80
CAP = 4
SLOTS = 96
SEQ = 1920
N_DP = 32
N_SEQ = 24


def draw_xact(key, part):
    full_shape = (N_DP, N_SEQ, SLOTS, PM, DV)
    key_base, key_rows, key_cols = jax.random.split(jax.random.fold_in(key, 17), 3)
    row_scale = jnp.exp(jax.random.uniform(key_rows, (N_DP, N_SEQ, SLOTS, PM, 1), jnp.float32, jnp.log(0.5), jnp.log(6.0)))
    col_scale = jnp.exp(jax.random.uniform(key_cols, (DV,), jnp.float32, jnp.log(0.3), jnp.log(3.0)))
    values = jnp.clip(jax.random.normal(key_base, full_shape, jnp.float32), -4.0, 4.0)
    return (values * row_scale * col_scale).astype(jnp.bfloat16)


def spiked(values, rng, source, target, parts, factor):
    def block_of(axis_at):
        return (jnp.arange(values.shape[axis_at]) // (values.shape[axis_at] // parts)).reshape((-1,) + (1,) * (values.ndim - 1 - axis_at))

    first = jax.random.permutation(rng, parts)[block_of(target)]
    far = (block_of(target) + parts // 2) % parts
    return jnp.where((block_of(source) == first) | (block_of(source) == far), factor * values, values)


def block_levels(stream_key, shape, cuts, smallest, high):
    def one(dim, shards_of):
        draws = jax.random.uniform(jax.random.fold_in(jax.random.fold_in(stream_key, 6), dim), (shards_of,), jnp.float32, smallest / len(cuts), high / len(cuts))
        return jnp.repeat(jnp.exp(draws), shape[dim] // shards_of).reshape((-1,) + (1,) * (len(shape) - dim - 1))

    level = one(*cuts[0])
    for cut in cuts[1:]:
        level = level * one(*cut)
    return level


def deal_out(own_key, own, number, rows, amount, top, reach, slope):
    sequence = jax.random.permutation(own_key, amount)
    crowded, ordinary = shares(amount, rows * top, reach, slope, True), shares(amount, rows * top, reach, slope, False)
    places = jnp.arange(amount)

    def named(sizes, turn):
        used = int((sizes > 0).sum())
        fixed = max(1, used // 4)
        moved = fixed + (places - fixed + turn * (used - fixed)) % max(1, amount - fixed)
        return jnp.zeros((amount,), jnp.int32).at[sequence[jnp.where(places < fixed, places, moved)]].set(jnp.asarray(sizes, jnp.int32))

    sizes = jnp.where(number % 4 == 0, named(crowded, number // 4), named(ordinary, number - number // 4 - 1))
    mixed = jax.random.permutation(jax.random.fold_in(own, 3), amount)
    giver, taker = mixed[0:amount // 2 * 2:2], mixed[1:amount // 2 * 2:2]
    margin = jnp.minimum(sizes[giver] - 1, reach - sizes[taker]) // 2
    margin = jnp.where((giver == sequence[0]) | (taker == sequence[0]) | (sizes[taker] == 0), 0, jnp.maximum(margin, 0))
    moved = jax.random.randint(jax.random.fold_in(own, 4), (amount // 2,), 0, 1 << 20) % (margin + 1)
    sizes = sizes.at[giver].add(-moved).at[taker].add(moved)
    labels = jnp.searchsorted(jnp.cumsum(sizes), jnp.arange(rows * top), side="right").astype(jnp.int32)
    listing = labels.reshape(top, rows).T
    listing = listing[jax.random.permutation(jax.random.fold_in(own, 1), rows)]
    turn = jax.random.randint(jax.random.fold_in(own, 2), (rows, 1), 0, top)
    return jnp.take_along_axis(listing, (jnp.arange(top)[None, :] + turn) % top, axis=1)


def shares(amount, total, most, slope, full):
    portions = [(1 << 20) // math.isqrt(grade ** slope) + 1 for grade in range(1, amount + 1)]
    largest = most if full else min(most, max(-(-total // amount), total * portions[0] // sum(portions)))
    least = 1 if total - largest >= amount - 1 else 0
    counts, spare = [largest] + [least] * (amount - 1), total - largest - least * (amount - 1)
    while spare > 0:
        free = [i for i in range(1, amount) if counts[i] < largest] or [i for i in range(1, amount) if counts[i] < most]
        whole, left = sum([portions[i] for i in free]), spare
        for i in free:
            addition = min(most - counts[i], max(1, left * portions[i] // whole), spare)
            counts[i] = counts[i] + addition
            spare = spare - addition
    return np.array(counts)


def scatter_about(key, shape, width, reach, cuts=(), kind=jnp.bfloat16):
    values = jax.random.normal(key, shape, jnp.float32) * width
    if len(cuts) > 0:
        values = block_levels(key, shape, cuts, -0.22, 0.18) * values
    return jnp.clip(values, min=-reach, max=reach).astype(kind)


def gaussian_with(key, dims, width, bound, shards, heavy, held_as=jnp.bfloat16):
    entries = width * jax.random.normal(key, dims, jnp.float32)
    if shards:
        entries = entries * block_levels(key, dims, shards, -0.22, 0.18)
    return jnp.clip(spiked(entries, jax.random.fold_in(key, 3), *heavy), -bound, bound).astype(held_as)


def setup_inputs(seed: int = 0) -> dict:
    splits = jax.random.split(jax.random.key(seed), 7)
    grad_rows = scatter_about(splits[0], (N_DP, SEQ, PM, DV), 1.0, 6.0, ((0, 32), (1, 24)))
    row_owner_keys = jax.random.split(jax.random.fold_in(splits[1], 1), N_DP * SEQ // TOK_DEV)
    row_owner_turns = jax.random.permutation(jax.random.fold_in(splits[1], 3), N_DP * SEQ // TOK_DEV)
    row_owner = jax.vmap(lambda own, number: deal_out(jax.random.fold_in(splits[1], 2), own, number, TOK_DEV, N_SEQ, 1, CAP, 2))(row_owner_keys, row_owner_turns).reshape((N_DP, SEQ, 1))
    acts = gaussian_with(splits[2], (N_DP, N_SEQ, SLOTS, PM, DV), 1.0, 6.0, ((0, 32), (1, 24)), (0, 4, 32, 2.75))
    xact = draw_xact(jax.random.fold_in(splits[6], 71), 0)
    gamma = jnp.clip(1.0 + 0.15 * jax.random.normal(splits[4], (DV,), jnp.float32), 0.25, 1.75)
    w_out = scatter_about(splits[5], (DV, DV), DV ** -0.5, 0.15625)
    return dict(grad_rows=grad_rows, row_owner=row_owner, acts=acts, xact=xact, gamma=gamma, w_out=w_out)


epsilon = 1e-06

def slot_table(owners, buckets, capacity):
    picked = (owners[:, None] == jnp.arange(buckets, dtype=jnp.int32)[None, :]).astype(jnp.int32)
    before = jnp.cumsum(picked, axis=0) - picked
    ranking = lax.optimization_barrier(jnp.sum(before * picked, axis=1)).astype(jnp.int32)
    target = owners.astype(jnp.int32) * capacity + ranking
    places = jnp.arange(buckets * capacity, dtype=jnp.int32)
    return (places[:, None] == target[None, :]).astype(jnp.bfloat16)

def norm_backward(upstream, inputs, gamma):
    values = inputs.astype(jnp.float32)
    inverse = lax.rsqrt(lax.optimization_barrier(jnp.mean(values * values, axis=1, keepdims=True)) + epsilon)
    normed = values * inverse
    gradient = upstream.astype(jnp.float32)
    gain_part = lax.optimization_barrier(jnp.sum(gradient * normed, axis=0))
    scaled = gamma.astype(jnp.float32) * gradient
    centre = lax.optimization_barrier(jnp.mean(scaled * normed, axis=1, keepdims=True))
    patch_grad = (inverse * (scaled - normed * centre)).astype(jnp.bfloat16)
    return (patch_grad, gain_part)

def reference(grad_rows, row_owner, acts, xact, gamma, w_out):

    def place(owner_block, row_block):
        placing = slot_table(owner_block, N_SEQ, CAP)
        return jnp.dot(placing, row_block, preferred_element_type=jnp.float32).astype(jnp.bfloat16)

    def group_terms(carry, group):
        grad_group, owner_group, acts_group, xact_group = group
        owners = owner_group[:, 0].reshape(N_SEQ, TOK_DEV)
        row_blocks = grad_group.reshape(N_SEQ, TOK_DEV, PM * DV)
        outgoing = jax.vmap(place)(owners, row_blocks).reshape(N_SEQ, N_SEQ, CAP, PM * DV)
        received = jnp.swapaxes(outgoing, 0, 1).reshape(N_SEQ * SLOTS * PM, DV)
        act_rows = acts_group.reshape(N_SEQ * SLOTS * PM, DV)
        patch_grad, gain_part = norm_backward(received, xact_group.reshape(N_SEQ * SLOTS * PM, DV), gamma)
        attn = lax.dot_general(patch_grad, w_out, (((1,), (1,)), ((), ())), preferred_element_type=jnp.float32).astype(jnp.bfloat16)
        weight_part = lax.dot_general(act_rows, patch_grad, (((0,), (0,)), ((), ())), preferred_element_type=jnp.float32)
        return ((carry[0] + weight_part, carry[1] + gain_part), attn.reshape(N_SEQ, SLOTS, PM, DV))
    initial = (jnp.zeros((DV, DV), jnp.float32), jnp.zeros((DV,), jnp.float32))
    totals, attn_grad = lax.scan(group_terms, initial, (grad_rows, row_owner, acts, xact))
    weight_raw, gain_raw = totals
    norm_total = jnp.sqrt(jnp.sum(weight_raw * weight_raw) + jnp.sum(gain_raw * gain_raw) + epsilon)
    factor = jnp.float32(DV) / norm_total
    return (attn_grad, weight_raw * factor, gain_raw * factor)
```

```python
import functools

import jax
import jax.numpy as jnp
from jax import lax
from jax.experimental import pallas as pl
from jax.experimental.pallas import tpu as pltpu
from jax.sharding import Mesh
from jax.sharding import PartitionSpec as P

DP = ("dp_0", "dp_1")
SEQ = ("z", "core")

epsilon = 1e-06


def copies(array, axes):
    count = lax.axis_size(axes)
    sent = jnp.broadcast_to(array[None], (count, *array.shape))
    return lax.all_to_all(sent, axes, 0, 0, tiled=True)


def summed_blocks(total, axis):
    count = lax.axis_size(axis)
    blocks = total.reshape(count, total.shape[0] // count, *total.shape[1:])
    return lax.all_to_all(blocks, axis, 0, 0, tiled=True).astype(jnp.float32).sum(0)


def slot_targets(owners, buckets, capacity):
    picked = (owners[:, None] == jnp.arange(buckets, dtype=jnp.int32)[None, :]).astype(jnp.int32)
    before = jnp.cumsum(picked, axis=0) - picked
    ranking = jnp.sum(before * picked, axis=1)
    return owners * capacity + ranking


def norm_kernel(step, core_ref, recv_ref, xact_ref, gamma_ref, grad_ref, keep_ref, send_ref, gain_ref):
    rows, features = recv_ref.shape
    half = features // 2
    mine = pl.multiple_of(core_ref[0] * half, half)
    other = pl.multiple_of((1 - core_ref[0]) * half, half)
    gain_ref[...] = jnp.zeros_like(gain_ref)
    gamma = gamma_ref[...]

    def body(i, carry):
        at = pl.ds(pl.multiple_of(i * step, step), step)
        values = xact_ref[at, :].astype(jnp.float32)
        gradient = recv_ref[at, :].astype(jnp.float32)
        inverse = lax.rsqrt(jnp.mean(values * values, axis=1, keepdims=True) + epsilon)
        normed = values * inverse
        gain_ref[...] += (gradient * normed).reshape(step // 8, 8, features).sum(0)
        scaled = gamma * gradient
        centre = jnp.mean(scaled * normed, axis=1, keepdims=True)
        grad_ref[at, :] = (inverse * (scaled - normed * centre)).astype(jnp.bfloat16)
        keep_ref[at, :] = grad_ref[at, pl.ds(mine, half)]
        send_ref[at, :] = grad_ref[at, pl.ds(other, half)]
        return carry

    lax.fori_loop(0, rows // step, body, 0)


def norm_backward(core, upstream, inputs, gamma):
    rows, features = upstream.shape
    whole = pl.BlockSpec(memory_space=pltpu.VMEM)
    return pl.pallas_call(
        functools.partial(norm_kernel, 16),
        out_shape=(
            jax.ShapeDtypeStruct((rows, features), jnp.bfloat16),
            jax.ShapeDtypeStruct((rows, features // 2), jnp.bfloat16),
            jax.ShapeDtypeStruct((rows, features // 2), jnp.bfloat16),
            jax.ShapeDtypeStruct((8, features), jnp.float32),
        ),
        in_specs=[pl.BlockSpec(memory_space=pltpu.SMEM), whole, whole, whole],
        out_specs=(whole, whole, whole, whole),
        name="norm_backward",
        compiler_params=pltpu.CompilerParams(vmem_limit_bytes=12 * 1024 * 1024),
        cost_estimate=pl.CostEstimate(flops=14 * rows * features, bytes_accessed=8 * rows * features, transcendentals=rows),
    )(core, upstream, inputs, gamma.reshape(1, features))


def on_device(grad_rows, row_owner, acts, xact, gamma, w_out):
    seq_count = lax.axis_size(SEQ)
    slot_count, patches, features = acts.shape[2:]
    capacity = slot_count // seq_count
    rows = slot_count * patches
    core = lax.axis_index("core")
    swap = [(0, 1), (1, 0)]

    target = slot_targets(row_owner[0, :, 0], seq_count, capacity)
    places = (target[:, None] * patches + jnp.arange(patches, dtype=jnp.int32)[None, :]).reshape(-1)
    placing = (jnp.arange(rows, dtype=jnp.int32)[:, None] == places[None, :]).astype(jnp.bfloat16)
    outgoing = jnp.dot(
        placing, grad_rows.reshape(-1, features), preferred_element_type=jnp.float32
    ).astype(jnp.bfloat16)
    received = lax.all_to_all(
        outgoing.reshape(seq_count, capacity * patches, features), SEQ, 0, 0, tiled=True
    ).reshape(rows, features)

    act_rows = acts.reshape(rows, features)
    act_pair = lax.ppermute(act_rows, "core", swap)
    xact_rows = xact.reshape(rows, features)

    grad, grad_keep, grad_send, gain_part = norm_backward(
        jnp.reshape(core, (1,)).astype(jnp.int32), received, xact_rows, gamma
    )
    grad_pair = lax.ppermute(grad_send, "core", swap)

    def outer(left, right):
        return lax.dot_general(left, right, (((0,), (0,)), ((), ())), preferred_element_type=jnp.float32)

    weight_pair = (outer(act_rows, grad_keep) + outer(act_pair, grad_pair)).astype(jnp.bfloat16)
    weight_x = summed_blocks(weight_pair, "dp_0").astype(jnp.bfloat16)
    attn_grad = lax.dot_general(
        grad, w_out, (((1,), (1,)), ((), ())), preferred_element_type=jnp.float32
    ).astype(jnp.bfloat16).reshape(acts.shape)
    weight_y = summed_blocks(weight_x, "dp_1")

    z_count = lax.axis_size("z")
    out_rows, half = weight_y.shape
    padded = -(-out_rows // z_count) * z_count
    weight_y = jnp.pad(weight_y, ((0, padded - out_rows), (0, 0))).astype(jnp.bfloat16)
    piece = summed_blocks(weight_y, "z")

    gain_seq = copies(gain_part.sum(0), SEQ).sum(0)
    squares = jnp.sum(piece * piece)
    pieces = copies(piece, SEQ).reshape(z_count, 2, padded // z_count, half)
    weight_sum = pieces.transpose(0, 2, 1, 3).reshape(padded, features)[:out_rows]
    squares = jnp.sum(weight_sum * weight_sum)
    both = copies(jnp.concatenate([gain_seq, jnp.full((128,), squares)]), DP).sum(0)
    gain_sum, square_total = both[:features], both[features]
    norm_total = jnp.sqrt(square_total + jnp.sum(gain_sum * gain_sum) + epsilon)
    factor = jnp.float32(features) / norm_total
    return (attn_grad, weight_sum * factor, gain_sum * factor)


def solution(mesh):
    finer = Mesh(mesh.devices.reshape(4, 8, mesh.shape["seq"] // 2, 2), (*DP, *SEQ))
    placed = (
        P(DP, SEQ, None, None),
        P(DP, SEQ, None),
        P(DP, SEQ, None, None, None),
        P(DP, SEQ, None, None, None),
        P(),
        P(),
    )
    return jax.shard_map(
        on_device,
        mesh=finer,
        in_specs=placed,
        out_specs=(P(DP, SEQ, None, None, None), P(DP, None), P()),
        check_vma=False,
    )
```

```python
import functools

import jax
import jax.numpy as jnp
from jax import lax
from jax.experimental import pallas as pl
from jax.experimental.pallas import tpu as pltpu
from jax.sharding import Mesh
from jax.sharding import PartitionSpec as P

DP = ("dp_0", "dp_1")
SEQ = ("z", "core")
LANES = 128

epsilon = 1e-06
f32 = jnp.float32
bf16 = jnp.bfloat16
VMEM = pl.BlockSpec(memory_space=pltpu.VMEM)
SMEM = pl.BlockSpec(memory_space=pltpu.SMEM)


def call(kernel, name, outs, ins, flops=0, limit=24):
    specs = [SMEM if a.shape == (1,) else VMEM for a in ins]
    moved = sum(a.size * a.dtype.itemsize for a in (*ins, *outs))
    return pl.pallas_call(
        kernel,
        name=name,
        out_shape=outs,
        in_specs=specs,
        out_specs=tuple(VMEM for _ in outs),
        compiler_params=pltpu.CompilerParams(vmem_limit_bytes=limit * 1024 * 1024),
        cost_estimate=pl.CostEstimate(flops=max(flops, 1000000), bytes_accessed=moved, transcendentals=0),
    )(*ins)


def exchange(blocks, axes):
    return lax.all_to_all(blocks, axes, 0, 0, tiled=True)


def iota(shape, dim):
    return lax.broadcasted_iota(jnp.int32, shape, dim)


def gather_kernel(buckets, capacity, patches, owner_ref, rows_ref, out_ref):
    count = owner_ref.shape[1]
    owner = owner_ref[...]
    picked = (iota((buckets, count), 0) == owner).astype(f32)
    earlier = (iota((count, count), 0) < iota((count, count), 1)).astype(f32)
    before = jnp.dot(picked.astype(bf16), earlier.astype(bf16), preferred_element_type=f32)
    ranking = jnp.sum(before * picked, axis=0, keepdims=True)
    target = owner.astype(f32) * capacity + ranking
    spread = (iota((count, count * patches), 0) == iota((count, count * patches), 1) // patches).astype(bf16)
    wide = jnp.dot(jnp.broadcast_to(target, (8, count)).astype(bf16), spread, preferred_element_type=f32)[:1]
    place = wide.astype(jnp.int32) * patches + iota((1, count * patches), 1) % patches
    total = out_ref.shape[0]
    placing = (iota((total, count * patches), 0) == place).astype(bf16)
    out_ref[...] = jnp.dot(placing, rows_ref[...], preferred_element_type=f32).astype(bf16)


def norm_kernel(step, core_ref, recv_ref, xact_ref, gamma_ref, grad_ref, keep_ref, send_ref, gain_ref, sum_ref):
    rows, features = recv_ref.shape
    half = features // 2
    mine = pl.multiple_of(core_ref[0] * half, half)
    other = pl.multiple_of((1 - core_ref[0]) * half, half)
    sum_ref[...] = jnp.zeros_like(sum_ref)
    gamma = gamma_ref[...]

    def body(i, carry):
        at = pl.ds(pl.multiple_of(i * step, step), step)
        values = xact_ref[at, :].astype(f32)
        gradient = recv_ref[at, :].astype(f32)
        inverse = lax.rsqrt(jnp.mean(values * values, axis=1, keepdims=True) + epsilon)
        normed = values * inverse
        sum_ref[...] += (gradient * normed).reshape(step // 8, 8, features).sum(0)
        scaled = gamma * gradient
        centre = jnp.mean(scaled * normed, axis=1, keepdims=True)
        grad_ref[at, :] = (inverse * (scaled - normed * centre)).astype(bf16)
        keep_ref[at, :] = grad_ref[at, pl.ds(mine, half)]
        send_ref[at, :] = grad_ref[at, pl.ds(other, half)]
        return carry

    lax.fori_loop(0, rows // step, body, 0)
    gain_ref[...] = jnp.sum(sum_ref[...], axis=0, keepdims=True)


def weight_kernel(left_ref, left_pair_ref, right_ref, right_pair_ref, gain_ref, out_ref):
    blocks, height, _ = out_ref.shape
    rows = height - 8
    gain = gain_ref[...]
    chunks = gain.shape[1] // LANES
    for b in range(blocks):
        at = slice(b * rows, (b + 1) * rows)
        out_ref[b, :rows, :] = (
            jnp.dot(left_ref[at, :], right_ref[...], preferred_element_type=f32)
            + jnp.dot(left_pair_ref[at, :], right_pair_ref[...], preferred_element_type=f32)
        ).astype(bf16)
        out_ref[b, rows:, :] = jnp.zeros((8, out_ref.shape[2]), bf16)
        lines = [
            gain[:, n * LANES:(n + 1) * LANES] if n < chunks else jnp.zeros((1, LANES), f32)
            for n in range(b * 8, b * 8 + 8)
        ]
        if b * 8 < chunks:
            out_ref[b, rows:, :LANES] = jnp.concatenate(lines, axis=0).astype(bf16)


def first_sum_kernel(in_ref, out_ref):
    blocks, height, width = out_ref.shape
    rows = height - 8
    lines = in_ref[:, blocks * rows:, :].astype(f32).sum(0)
    for b in range(blocks):
        out_ref[b, :rows, :] = in_ref[:, b * rows:(b + 1) * rows, :].astype(f32).sum(0).astype(bf16)
        own = jnp.where(iota((8, width), 0) == 0, lines[b:b + 1, :], 0.0)
        out_ref[b, rows:, :] = own.astype(bf16)


def second_sum_kernel(in_ref, out_ref):
    total = in_ref[...].astype(f32).sum(0)
    pieces, height, _ = out_ref.shape
    for b in range(pieces):
        out_ref[b] = total[b * height:(b + 1) * height, :].astype(bf16)


def third_sum_kernel(in_ref, out_ref):
    total = in_ref[...].astype(f32).sum(0)
    for b in range(out_ref.shape[0]):
        out_ref[b] = total


def joined_kernel(in_ref, weight_ref, note_ref):
    pieces, height, half = in_ref.shape
    rows = weight_ref.shape[0]
    squares = jnp.zeros((height, half), f32)
    for p in range(pieces):
        at = (p // 2) * height
        if at < rows:
            block = in_ref[p]
            squares += block * block
            weight_ref[at:at + height, (p % 2) * half:(p % 2 + 1) * half] = block
    p = 2 * (rows // height)
    gain = in_ref[p, :1, :LANES] + in_ref[p + 1, :1, :LANES]
    line = jnp.concatenate([gain, jnp.full((1, LANES), jnp.sum(squares), f32)], axis=1)
    for d in range(note_ref.shape[0]):
        note_ref[d] = line


def scale_kernel(features, note_ref, weight_ref, weight_out_ref, gain_out_ref):
    chunks = features // LANES
    notes = note_ref[...]
    squares = jnp.sum(jnp.max(notes[:, :, LANES:], axis=2))
    gain = notes[:chunks, :, :LANES]
    total = squares + jnp.sum(gain * gain)
    factor = f32(features) * lax.rsqrt(jnp.full((1, LANES), total + epsilon, f32))
    for n in range(chunks):
        gain_out_ref[:, n * LANES:(n + 1) * LANES] = gain[n] * factor
        at = slice(n * LANES, (n + 1) * LANES)
        weight_out_ref[:, at] = weight_ref[:, at] * factor


def on_device(grad_rows, row_owner, acts, xact, gamma, w_out):
    seq_count = lax.axis_size(SEQ)
    x_count, y_count, z_count = (lax.axis_size(a) for a in ("dp_0", "dp_1", "z"))
    tokens = row_owner.shape[1]
    slot_count, patches, features = acts.shape[2:]
    capacity = slot_count // seq_count
    rows = slot_count * patches
    half = features // 2
    core = jnp.reshape(lax.axis_index("core"), (1,)).astype(jnp.int32)
    swap = [(0, 1), (1, 0)]

    def shaped(dtype, *shape):
        return jax.ShapeDtypeStruct(shape, dtype)

    (outgoing,) = call(
        functools.partial(gather_kernel, seq_count, capacity, patches),
        "gather_rows",
        (shaped(bf16, rows, features),),
        (row_owner.reshape(1, tokens), grad_rows.reshape(tokens * patches, features)),
    )
    received = exchange(outgoing.reshape(seq_count, capacity * patches, features), SEQ)

    act_rows = acts.reshape(rows, features)
    act_pair = lax.ppermute(act_rows, "core", swap)
    left, left_pair, xact_rows = lax.optimization_barrier(
        (act_rows.T, act_pair.T, xact.reshape(rows, features))
    )

    grad, grad_keep, grad_send, gain_part, _ = call(
        functools.partial(norm_kernel, 16),
        "norm_backward",
        (
            shaped(bf16, rows, features),
            shaped(bf16, rows, half),
            shaped(bf16, rows, half),
            shaped(f32, 1, features),
            shaped(f32, 8, features),
        ),
        (core, received.reshape(rows, features), xact_rows, gamma.reshape(1, features)),
    )
    grad_pair = lax.ppermute(grad_send, "core", swap)

    x_rows = features // x_count
    y_rows = x_rows // y_count
    z_rows = (y_rows + 8) // z_count
    (weight_pair,) = call(
        weight_kernel,
        "weight_pair",
        (shaped(bf16, x_count, x_rows + 8, half),),
        (left, left_pair, grad_keep, grad_pair, gain_part),
        flops=4 * features * half * rows,
    )
    (weight_x,) = call(
        first_sum_kernel,
        "sum_first",
        (shaped(bf16, y_count, y_rows + 8, half),),
        (exchange(weight_pair, "dp_0"),),
    )
    (weight_y,) = call(
        second_sum_kernel,
        "sum_second",
        (shaped(bf16, z_count, z_rows, half),),
        (exchange(weight_x, "dp_1"),),
    )
    (pieces,) = call(
        third_sum_kernel,
        "sum_third",
        (shaped(f32, seq_count, z_rows, half),),
        (exchange(weight_y, "z"),),
    )
    weight_sum, note = call(
        joined_kernel,
        "joined",
        (shaped(f32, y_rows, features), shaped(f32, x_count * y_count, 1, 2 * LANES)),
        (exchange(pieces, SEQ),),
    )
    attn_grad = lax.dot_general(
        grad, w_out, (((1,), (1,)), ((), ())), preferred_element_type=f32
    ).astype(bf16).reshape(acts.shape)
    weight_grad, gain_grad = call(
        functools.partial(scale_kernel, features),
        "scaled",
        (shaped(f32, y_rows, features), shaped(f32, 1, features)),
        (exchange(note, DP), weight_sum),
    )
    return (attn_grad, weight_grad, gain_grad.reshape(features))


def solution(mesh):
    finer = Mesh(mesh.devices.reshape(4, 8, mesh.shape["seq"] // 2, 2), (*DP, *SEQ))
    placed = (
        P(DP, SEQ, None, None),
        P(DP, SEQ, None),
        P(DP, SEQ, None, None, None),
        P(DP, SEQ, None, None, None),
        P(),
        P(),
    )
    return jax.shard_map(
        on_device,
        mesh=finer,
        in_specs=placed,
        out_specs=(P(DP, SEQ, None, None, None), P(DP, None), P()),
        check_vma=False,
    )
```

```python
import functools

import jax
import jax.numpy as jnp
from jax import lax
from jax.experimental import pallas as pl
from jax.experimental.pallas import tpu as pltpu
from jax.sharding import Mesh
from jax.sharding import PartitionSpec as P

DP = ("dp_0", "dp_1")
SEQ = ("z", "core")
LANES = 128

epsilon = 1e-06
f32 = jnp.float32
bf16 = jnp.bfloat16
VMEM = pl.BlockSpec(memory_space=pltpu.VMEM)
SMEM = pl.BlockSpec(memory_space=pltpu.SMEM)
FAR = pl.BlockSpec(memory_space=pltpu.HBM)


def call(kernel, name, outs, ins, flops=0, limit=24, far_in=(), far_out=(), scratch=()):
    specs = [SMEM if a.shape == (1,) else (FAR if n in far_in else VMEM) for n, a in enumerate(ins)]
    moved = sum(a.size * a.dtype.itemsize for a in (*ins, *outs))
    return pl.pallas_call(
        kernel,
        name=name,
        out_shape=outs,
        in_specs=specs,
        out_specs=tuple(FAR if n in far_out else VMEM for n in range(len(outs))),
        scratch_shapes=scratch,
        compiler_params=pltpu.CompilerParams(vmem_limit_bytes=limit * 1024 * 1024),
        cost_estimate=pl.CostEstimate(flops=max(flops, 1000000), bytes_accessed=moved, transcendentals=0),
    )(*ins)


def exchange(blocks, axes):
    return lax.all_to_all(blocks, axes, 0, 0, tiled=True)


def iota(shape, dim):
    return lax.broadcasted_iota(jnp.int32, shape, dim)


def gather_kernel(buckets, capacity, patches, chunks, owner_ref, rows_ref, out_ref, hold_ref, sems):
    count = owner_ref.shape[1]
    features = rows_ref.shape[2]
    owner = owner_ref[...]
    picked = (iota((buckets, count), 0) == owner).astype(f32)
    earlier = (iota((count, count), 0) < iota((count, count), 1)).astype(f32)
    before = jnp.dot(picked.astype(bf16), earlier.astype(bf16), preferred_element_type=f32)
    ranking = jnp.sum(before * picked, axis=0, keepdims=True)
    target = owner.astype(f32) * capacity + ranking
    spread = (iota((count, count * patches), 0) == iota((count, count * patches), 1) // patches).astype(bf16)
    wide = jnp.dot(jnp.broadcast_to(target, (8, count)).astype(bf16), spread, preferred_element_type=f32)[:1]
    place = wide.astype(jnp.int32) * patches + iota((1, count * patches), 1) % patches
    lines = rows_ref[...].reshape(count * patches, features)
    step = out_ref.shape[0] // chunks
    copies = []
    for n in range(chunks):
        placing = (iota((step, count * patches), 0) + n * step == place).astype(bf16)
        at = pl.ds(n * step, step)
        hold_ref[at, :] = jnp.dot(placing, lines, preferred_element_type=f32).astype(bf16)
        copies.append(pltpu.make_async_copy(hold_ref.at[at, :], out_ref.at[at, :], sems.at[n]))
        copies[-1].start()
    for copy in copies:
        copy.wait()


def prepare_kernel(step, xact_ref, acts_ref, pair_ref, lines_ref, inverse_ref, left_ref, left_pair_ref):
    slots, patches, features = xact_ref.shape
    height = step * patches
    for n in range(slots // step):
        at = slice(n * height, (n + 1) * height)
        lines = xact_ref[n * step:(n + 1) * step].reshape(height, features)
        lines_ref[at, :] = lines
        values = lines.astype(f32)
        inverse_ref[at, :] = lax.rsqrt(jnp.mean(values * values, axis=1, keepdims=True) + epsilon)
    for source, target in ((acts_ref, left_ref), (pair_ref, left_pair_ref)):
        width = LANES
        for n in range(slots * patches // width):
            block = source[n * width // patches:(n + 1) * width // patches].reshape(width, features)
            target[:, n * width:(n + 1) * width] = block.T


def norm_kernel(
    chunks, step, core_ref, recv_ref, lines_ref, inverse_ref, gamma_ref,
    grad_ref, keep_ref, send_ref, gain_ref, hold_ref, values_ref, made_ref, in_sems, value_sems, out_sems,
):
    rows, features = recv_ref.shape
    half = features // 2
    height = rows // chunks
    first = core_ref[0] == 0
    gamma = gamma_ref[...]
    incoming = []
    for n in range(chunks):
        at = pl.ds(n * height, height)
        incoming.append((
            pltpu.make_async_copy(recv_ref.at[at, :], hold_ref.at[at, :], in_sems.at[n]),
            pltpu.make_async_copy(lines_ref.at[at, :], values_ref.at[at, :], value_sems.at[n]),
        ))
        for copy in incoming[-1]:
            copy.start()

    def body(i, gain):
        at = pl.ds(pl.multiple_of(i * step, step), step)
        inverse = inverse_ref[at, :]
        normed = values_ref[at, :].astype(f32) * inverse
        gradient = hold_ref[at, :].astype(f32)
        both = gradient * normed
        gain = gain + both.reshape(step // 8, 8, features).sum(0)
        centre = jnp.mean(gamma * both, axis=1, keepdims=True)
        made = (inverse * (gamma * gradient - normed * centre)).astype(bf16)
        made_ref[at, :] = made
        low, high = made[:, :half], made[:, half:]
        keep_ref[at, :] = jnp.where(first, low, high)
        send_ref[at, :] = jnp.where(first, high, low)
        return gain

    gain = jnp.zeros((8, features), f32)
    outgoing = []
    for n in range(chunks):
        at = pl.ds(n * height, height)
        for copy in incoming[n]:
            copy.wait()
        gain = lax.fori_loop(n * height // step, (n + 1) * height // step, body, gain, unroll=2)
        outgoing.append(pltpu.make_async_copy(made_ref.at[at, :], grad_ref.at[at, :], out_sems.at[n]))
        outgoing[-1].start()
    gain_ref[...] = jnp.sum(gain, axis=0, keepdims=True)
    for copy in outgoing:
        copy.wait()


def weight_kernel(left_ref, left_pair_ref, right_ref, right_pair_ref, gain_ref, out_ref):
    blocks, height, _ = out_ref.shape
    rows = height - 8
    gain = gain_ref[...]
    chunks = gain.shape[1] // LANES
    for b in range(blocks):
        at = slice(b * rows, (b + 1) * rows)
        out_ref[b, :rows, :] = (
            jnp.dot(left_ref[at, :], right_ref[...], preferred_element_type=f32)
            + jnp.dot(left_pair_ref[at, :], right_pair_ref[...], preferred_element_type=f32)
        ).astype(bf16)
        out_ref[b, rows:, :] = jnp.zeros((8, out_ref.shape[2]), bf16)
        lines = [
            gain[:, n * LANES:(n + 1) * LANES] if n < chunks else jnp.zeros((1, LANES), f32)
            for n in range(b * 8, b * 8 + 8)
        ]
        if b * 8 < chunks:
            out_ref[b, rows:, :LANES] = jnp.concatenate(lines, axis=0).astype(bf16)


def first_sum_kernel(in_ref, out_ref):
    blocks, height, width = out_ref.shape
    rows = height - 8
    lines = in_ref[:, blocks * rows:, :].astype(f32).sum(0)
    for b in range(blocks):
        out_ref[b, :rows, :] = in_ref[:, b * rows:(b + 1) * rows, :].astype(f32).sum(0).astype(bf16)
        own = jnp.where(iota((8, width), 0) == 0, lines[b:b + 1, :], 0.0)
        out_ref[b, rows:, :] = own.astype(bf16)


def second_sum_kernel(in_ref, out_ref):
    total = in_ref[...].astype(f32).sum(0)
    pieces, height, _ = out_ref.shape
    for b in range(pieces):
        out_ref[b] = total[b * height:(b + 1) * height, :].astype(bf16)


def third_sum_kernel(in_ref, out_ref):
    total = in_ref[...].astype(f32).sum(0)
    total = total.astype(bf16)
    for b in range(out_ref.shape[0]):
        out_ref[b] = total


def joined_kernel(in_ref, weight_ref, note_ref):
    pieces, height, half = in_ref.shape
    rows = weight_ref.shape[0]
    squares = jnp.zeros((height, half), f32)
    for p in range(pieces):
        at = (p // 2) * height
        if at < rows:
            block = in_ref[p].astype(f32)
            squares += block * block
            weight_ref[at:at + height, (p % 2) * half:(p % 2 + 1) * half] = block
    p = 2 * (rows // height)
    gain = (in_ref[p].astype(f32) + in_ref[p + 1].astype(f32))[:1, :LANES]
    line = jnp.concatenate([gain, jnp.full((1, LANES), jnp.sum(squares), f32)], axis=1)
    for d in range(note_ref.shape[0]):
        note_ref[d] = line


def scale_kernel(features, note_ref, weight_ref, weight_out_ref, gain_out_ref):
    chunks = features // LANES
    notes = note_ref[...]
    squares = jnp.sum(jnp.max(notes[:, :, LANES:], axis=2))
    gain = notes[:chunks, :, :LANES]
    total = squares + jnp.sum(gain * gain)
    factor = f32(features) * lax.rsqrt(jnp.full((1, LANES), total + epsilon, f32))
    for n in range(chunks):
        gain_out_ref[:, n * LANES:(n + 1) * LANES] = gain[n] * factor
        at = slice(n * LANES, (n + 1) * LANES)
        weight_out_ref[:, at] = weight_ref[:, at] * factor


def on_device(grad_rows, row_owner, acts, xact, gamma, w_out):
    seq_count = lax.axis_size(SEQ)
    x_count, y_count, z_count = (lax.axis_size(a) for a in ("dp_0", "dp_1", "z"))
    tokens = row_owner.shape[1]
    slot_count, patches, features = acts.shape[2:]
    capacity = slot_count // seq_count
    rows = slot_count * patches
    half = features // 2
    core = jnp.reshape(lax.axis_index("core"), (1,)).astype(jnp.int32)
    swap = [(0, 1), (1, 0)]

    def shaped(dtype, *shape):
        return jax.ShapeDtypeStruct(shape, dtype)

    chunks = 3
    (outgoing,) = call(
        functools.partial(gather_kernel, seq_count, capacity, patches, chunks),
        "gather_rows",
        (shaped(bf16, rows, features),),
        (row_owner.reshape(1, tokens), grad_rows.reshape(tokens, patches, features)),
        far_out=(0,),
        limit=60,
        scratch=[pltpu.VMEM((rows, features), bf16), pltpu.SemaphoreType.DMA((chunks,))],
    )
    received = exchange(outgoing.reshape(seq_count, capacity * patches, features), SEQ)

    act_slots = acts.reshape(slot_count, patches, features)
    act_pair = lax.ppermute(act_slots, "core", swap)
    lines, inverse, left, left_pair = call(
        functools.partial(prepare_kernel, 8),
        "prepare",
        (
            shaped(bf16, rows, features),
            shaped(f32, rows, 1),
            shaped(bf16, features, rows),
            shaped(bf16, features, rows),
        ),
        (xact.reshape(slot_count, patches, features), act_slots, act_pair),
    )

    chunks = 6
    grad, grad_keep, grad_send, gain_part = call(
        functools.partial(norm_kernel, chunks, 16),
        "norm_backward",
        (
            shaped(bf16, rows, features),
            shaped(bf16, rows, half),
            shaped(bf16, rows, half),
            shaped(f32, 1, features),
        ),
        (core, received.reshape(rows, features), lines, inverse, gamma.reshape(1, features)),
        far_in=(1, 2),
        far_out=(0,),
        scratch=[
            pltpu.VMEM((rows, features), bf16),
            pltpu.VMEM((rows, features), bf16),
            pltpu.VMEM((rows, features), bf16),
            pltpu.SemaphoreType.DMA((chunks,)),
            pltpu.SemaphoreType.DMA((chunks,)),
            pltpu.SemaphoreType.DMA((chunks,)),
        ],
    )
    grad_pair = lax.ppermute(grad_send, "core", swap)

    x_rows = features // x_count
    y_rows = x_rows // y_count
    z_rows = (y_rows + 8) // z_count
    (weight_pair,) = call(
        weight_kernel,
        "weight_pair",
        (shaped(bf16, x_count, x_rows + 8, half),),
        (left, left_pair, grad_keep, grad_pair, gain_part),
        flops=4 * features * half * rows,
    )
    (weight_x,) = call(
        first_sum_kernel,
        "sum_first",
        (shaped(bf16, y_count, y_rows + 8, half),),
        (exchange(weight_pair, "dp_0"),),
    )
    (weight_y,) = call(
        second_sum_kernel,
        "sum_second",
        (shaped(bf16, z_count, z_rows, half),),
        (exchange(weight_x, "dp_1"),),
    )
    (pieces,) = call(
        third_sum_kernel,
        "sum_third",
        (shaped(bf16, seq_count, z_rows, half),),
        (exchange(weight_y, "z"),),
    )
    weight_sum, note = call(
        joined_kernel,
        "joined",
        (shaped(f32, y_rows, features), shaped(f32, x_count * y_count, 1, 2 * LANES)),
        (exchange(pieces, SEQ),),
    )
    attn_grad = lax.dot_general(
        grad, w_out, (((1,), (1,)), ((), ())), preferred_element_type=f32
    ).astype(bf16).reshape(acts.shape)
    weight_grad, gain_grad = call(
        functools.partial(scale_kernel, features),
        "scaled",
        (shaped(f32, y_rows, features), shaped(f32, 1, features)),
        (exchange(note, DP), weight_sum),
    )
    return (attn_grad, weight_grad, gain_grad.reshape(features))


def solution(mesh):
    finer = Mesh(mesh.devices.reshape(4, 8, mesh.shape["seq"] // 2, 2), (*DP, *SEQ))
    placed = (
        P(DP, SEQ, None, None),
        P(DP, SEQ, None),
        P(DP, SEQ, None, None, None),
        P(DP, SEQ, None, None, None),
        P(),
        P(),
    )
    return jax.shard_map(
        on_device,
        mesh=finer,
        in_specs=placed,
        out_specs=(P(DP, SEQ, None, None, None), P(DP, None), P()),
        check_vma=False,
    )
```

```python
import functools

import jax
import jax.numpy as jnp
from jax import lax
from jax.experimental import pallas as pl
from jax.experimental.pallas import tpu as pltpu
from jax.sharding import Mesh
from jax.sharding import PartitionSpec as P

DP = ("dp_0", "dp_1")
SEQ = ("z", "core")
LANES = 128

epsilon = 1e-06
f32 = jnp.float32
bf16 = jnp.bfloat16
VMEM = pl.BlockSpec(memory_space=pltpu.VMEM)
SMEM = pl.BlockSpec(memory_space=pltpu.SMEM)
FAR = pl.BlockSpec(memory_space=pltpu.HBM)


def call(kernel, name, outs, ins, flops=0, limit=24, far_in=(), far_out=(), scratch=()):
    specs = [SMEM if a.shape == (1,) else (FAR if n in far_in else VMEM) for n, a in enumerate(ins)]
    moved = sum(a.size * a.dtype.itemsize for a in (*ins, *outs))
    return pl.pallas_call(
        kernel,
        name=name,
        out_shape=outs,
        in_specs=specs,
        out_specs=tuple(FAR if n in far_out else VMEM for n in range(len(outs))),
        scratch_shapes=scratch,
        compiler_params=pltpu.CompilerParams(vmem_limit_bytes=limit * 1024 * 1024),
        cost_estimate=pl.CostEstimate(flops=max(flops, 1000000), bytes_accessed=moved, transcendentals=0),
    )(*ins)


def exchange(blocks, axes):
    return lax.all_to_all(blocks, axes, 0, 0, tiled=True)


def iota(shape, dim):
    return lax.broadcasted_iota(jnp.int32, shape, dim)


def gather_kernel(buckets, capacity, patches, chunks, owner_ref, rows_ref, out_ref, hold_ref, sems):
    count = owner_ref.shape[1]
    features = rows_ref.shape[2]
    owner = owner_ref[...]
    picked = (iota((buckets, count), 0) == owner).astype(f32)
    earlier = (iota((count, count), 0) < iota((count, count), 1)).astype(f32)
    before = jnp.dot(picked.astype(bf16), earlier.astype(bf16), preferred_element_type=f32)
    ranking = jnp.sum(before * picked, axis=0, keepdims=True)
    target = owner.astype(f32) * capacity + ranking
    spread = (iota((count, count * patches), 0) == iota((count, count * patches), 1) // patches).astype(bf16)
    wide = jnp.dot(jnp.broadcast_to(target, (8, count)).astype(bf16), spread, preferred_element_type=f32)[:1]
    place = wide.astype(jnp.int32) * patches + iota((1, count * patches), 1) % patches
    lines = rows_ref[...].reshape(count * patches, features)
    step = out_ref.shape[0] // chunks
    copies = []
    for n in range(chunks):
        placing = (iota((step, count * patches), 0) + n * step == place).astype(bf16)
        at = pl.ds(n * step, step)
        hold_ref[at, :] = jnp.dot(placing, lines, preferred_element_type=f32).astype(bf16)
        copies.append(pltpu.make_async_copy(hold_ref.at[at, :], out_ref.at[at, :], sems.at[n]))
        copies[-1].start()
    for copy in copies:
        copy.wait()


def prepare_kernel(step, xact_ref, acts_ref, pair_ref, lines_ref, inverse_ref, left_ref, left_pair_ref):
    slots, patches, features = xact_ref.shape
    height = step * patches
    for n in range(slots // step):
        at = slice(n * height, (n + 1) * height)
        lines = xact_ref[n * step:(n + 1) * step].reshape(height, features)
        lines_ref[at, :] = lines
        values = lines.astype(f32)
        inverse_ref[at, :] = lax.rsqrt(jnp.mean(values * values, axis=1, keepdims=True) + epsilon)
    for source, target in ((acts_ref, left_ref), (pair_ref, left_pair_ref)):
        width = LANES
        for n in range(slots * patches // width):
            block = source[n * width // patches:(n + 1) * width // patches].reshape(width, features)
            target[:, n * width:(n + 1) * width] = block.T


def norm_kernel(
    chunks, step, core_ref, recv_ref, lines_ref, left_ref, left_pair_ref, inverse_ref, gamma_ref,
    keep_ref, send_ref, left_out_ref, left_pair_out_ref, gain_ref, hold_ref, values_ref, sems, left_sems,
):
    rows, features = recv_ref.shape
    half = features // 2
    height = rows // chunks
    first = core_ref[0] == 0
    gamma = gamma_ref[...]
    incoming = []
    for n in range(chunks):
        at = pl.ds(n * height, height)
        incoming.append((
            pltpu.make_async_copy(recv_ref.at[at, :], hold_ref.at[at, :], sems.at[2 * n]),
            pltpu.make_async_copy(lines_ref.at[at, :], values_ref.at[at, :], sems.at[2 * n + 1]),
        ))
        for copy in incoming[-1]:
            copy.start()
    lefts = (
        pltpu.make_async_copy(left_ref, left_out_ref, left_sems.at[0]),
        pltpu.make_async_copy(left_pair_ref, left_pair_out_ref, left_sems.at[1]),
    )
    for copy in lefts:
        copy.start()

    def body(i, gain):
        at = pl.ds(pl.multiple_of(i * step, step), step)
        inverse = inverse_ref[at, :]
        normed = values_ref[at, :].astype(f32) * inverse
        gradient = hold_ref[at, :].astype(f32)
        both = gradient * normed
        gain = gain + both.reshape(step // 8, 8, features).sum(0)
        centre = jnp.mean(gamma * both, axis=1, keepdims=True)
        made = (inverse * (gamma * gradient - normed * centre)).astype(bf16)
        low, high = made[:, :half], made[:, half:]
        keep_ref[at, :] = jnp.where(first, low, high)
        send_ref[at, :] = jnp.where(first, high, low)
        return gain

    gain = jnp.zeros((8, features), f32)
    for n in range(chunks):
        for copy in incoming[n]:
            copy.wait()
        gain = lax.fori_loop(n * height // step, (n + 1) * height // step, body, gain, unroll=2)
    gain_ref[...] = jnp.sum(gain, axis=0, keepdims=True)
    for copy in lefts:
        copy.wait()


def whole_kernel(core_ref, keep_ref, send_ref, grad_ref):
    half = keep_ref.shape[1]
    first = core_ref[0] == 0
    keep, send = keep_ref[...], send_ref[...]
    grad_ref[:, :half] = jnp.where(first, keep, send)
    grad_ref[:, half:] = jnp.where(first, send, keep)


def weight_kernel(left_ref, left_pair_ref, right_ref, right_pair_ref, gain_ref, out_ref):
    blocks, height, _ = out_ref.shape
    rows = height - 8
    gain = gain_ref[...]
    chunks = gain.shape[1] // LANES
    for b in range(blocks):
        at = slice(b * rows, (b + 1) * rows)
        out_ref[b, :rows, :] = (
            jnp.dot(left_ref[at, :], right_ref[...], preferred_element_type=f32)
            + jnp.dot(left_pair_ref[at, :], right_pair_ref[...], preferred_element_type=f32)
        ).astype(bf16)
        out_ref[b, rows:, :] = jnp.zeros((8, out_ref.shape[2]), bf16)
        lines = [
            gain[:, n * LANES:(n + 1) * LANES] if n < chunks else jnp.zeros((1, LANES), f32)
            for n in range(b * 8, b * 8 + 8)
        ]
        if b * 8 < chunks:
            out_ref[b, rows:, :LANES] = jnp.concatenate(lines, axis=0).astype(bf16)


def first_sum_kernel(in_ref, out_ref):
    blocks, height, width = out_ref.shape
    rows = height - 8
    lines = in_ref[:, blocks * rows:, :].astype(f32).sum(0)
    for b in range(blocks):
        out_ref[b, :rows, :] = in_ref[:, b * rows:(b + 1) * rows, :].astype(f32).sum(0).astype(bf16)
        own = jnp.where(iota((8, width), 0) == 0, lines[b:b + 1, :], 0.0)
        out_ref[b, rows:, :] = own.astype(bf16)


def second_sum_kernel(in_ref, out_ref):
    total = in_ref[...].astype(f32).sum(0)
    pieces, height, _ = out_ref.shape
    for b in range(pieces):
        out_ref[b] = total[b * height:(b + 1) * height, :].astype(bf16)


def third_sum_kernel(in_ref, out_ref):
    total = in_ref[...].astype(f32).sum(0)
    total = total.astype(bf16)
    for b in range(out_ref.shape[0]):
        out_ref[b] = total


def joined_kernel(in_ref, weight_ref, note_ref):
    pieces, height, half = in_ref.shape
    rows = weight_ref.shape[0]
    squares = jnp.zeros((height, half), f32)
    for p in range(pieces):
        at = (p // 2) * height
        if at < rows:
            block = in_ref[p].astype(f32)
            squares += block * block
            weight_ref[at:at + height, (p % 2) * half:(p % 2 + 1) * half] = block
    p = 2 * (rows // height)
    gain = (in_ref[p].astype(f32) + in_ref[p + 1].astype(f32))[:1, :LANES]
    line = jnp.concatenate([gain, jnp.full((1, LANES), jnp.sum(squares), f32)], axis=1)
    for d in range(note_ref.shape[0]):
        note_ref[d] = line


def scale_kernel(features, note_ref, weight_ref, weight_out_ref, gain_out_ref):
    chunks = features // LANES
    notes = note_ref[...]
    squares = jnp.sum(jnp.max(notes[:, :, LANES:], axis=2))
    gain = notes[:chunks, :, :LANES]
    total = squares + jnp.sum(gain * gain)
    factor = f32(features) * lax.rsqrt(jnp.full((1, LANES), total + epsilon, f32))
    for n in range(chunks):
        gain_out_ref[n * LANES:(n + 1) * LANES] = (gain[n] * factor)[0]
        at = slice(n * LANES, (n + 1) * LANES)
        weight_out_ref[:, at] = weight_ref[:, at] * factor


def on_device(grad_rows, row_owner, acts, xact, gamma, w_out):
    seq_count = lax.axis_size(SEQ)
    x_count, y_count, z_count = (lax.axis_size(a) for a in ("dp_0", "dp_1", "z"))
    tokens = row_owner.shape[1]
    slot_count, patches, features = acts.shape[2:]
    capacity = slot_count // seq_count
    rows = slot_count * patches
    half = features // 2
    core = jnp.reshape(lax.axis_index("core"), (1,)).astype(jnp.int32)
    swap = [(0, 1), (1, 0)]

    def shaped(dtype, *shape):
        return jax.ShapeDtypeStruct(shape, dtype)

    chunks = 3
    (outgoing,) = call(
        functools.partial(gather_kernel, seq_count, capacity, patches, chunks),
        "gather_rows",
        (shaped(bf16, rows, features),),
        (row_owner.reshape(1, tokens), grad_rows.reshape(tokens, patches, features)),
        far_out=(0,),
        limit=60,
        scratch=[pltpu.VMEM((rows, features), bf16), pltpu.SemaphoreType.DMA((chunks,))],
    )
    received = exchange(outgoing.reshape(seq_count, capacity * patches, features), SEQ)

    act_slots = acts.reshape(slot_count, patches, features)
    act_pair = lax.ppermute(act_slots, "core", swap)
    lines, inverse, left, left_pair = call(
        functools.partial(prepare_kernel, 8),
        "prepare",
        (
            shaped(bf16, rows, features),
            shaped(f32, rows, 1),
            shaped(bf16, features, rows),
            shaped(bf16, features, rows),
        ),
        (xact.reshape(slot_count, patches, features), act_slots, act_pair),
    )

    chunks = 4
    grad_keep, grad_send, left, left_pair, gain_part = call(
        functools.partial(norm_kernel, chunks, 16),
        "norm_backward",
        (
            shaped(bf16, rows, half),
            shaped(bf16, rows, half),
            shaped(bf16, features, rows),
            shaped(bf16, features, rows),
            shaped(f32, 1, features),
        ),
        (core, received.reshape(rows, features), lines, left, left_pair, inverse, gamma.reshape(1, features)),
        far_in=(1, 2, 3, 4),
        limit=50,
        scratch=[
            pltpu.VMEM((rows, features), bf16),
            pltpu.VMEM((rows, features), bf16),
            pltpu.SemaphoreType.DMA((2 * chunks,)),
            pltpu.SemaphoreType.DMA((2,)),
        ],
    )
    grad_pair = lax.ppermute(grad_send, "core", swap)
    (grad,) = call(
        whole_kernel, "whole_grad", (shaped(bf16, rows, features),), (core, grad_keep, grad_send), limit=52
    )
    grad, grad_keep = lax.optimization_barrier((grad, grad_keep))

    x_rows = features // x_count
    y_rows = x_rows // y_count
    z_rows = (y_rows + 8) // z_count
    (weight_pair,) = call(
        weight_kernel,
        "weight_pair",
        (shaped(bf16, x_count, x_rows + 8, half),),
        (left, left_pair, grad_keep, grad_pair, gain_part),
        flops=4 * features * half * rows,
    )
    (weight_x,) = call(
        first_sum_kernel,
        "sum_first",
        (shaped(bf16, y_count, y_rows + 8, half),),
        (exchange(weight_pair, "dp_0"),),
    )
    (weight_y,) = call(
        second_sum_kernel,
        "sum_second",
        (shaped(bf16, z_count, z_rows, half),),
        (exchange(weight_x, "dp_1"),),
    )
    (pieces,) = call(
        third_sum_kernel,
        "sum_third",
        (shaped(bf16, seq_count, z_rows, half),),
        (exchange(weight_y, "z"),),
    )
    weight_sum, note = call(
        joined_kernel,
        "joined",
        (shaped(f32, y_rows, features), shaped(f32, x_count * y_count, 1, 2 * LANES)),
        (exchange(pieces, SEQ),),
    )
    attn_grad = lax.dot_general(
        grad, w_out, (((1,), (1,)), ((), ())), preferred_element_type=f32
    ).astype(bf16).reshape(acts.shape)
    weight_grad, gain_grad = call(
        functools.partial(scale_kernel, features),
        "scaled",
        (shaped(f32, y_rows, features), shaped(f32, features)),
        (exchange(note, DP), weight_sum),
    )
    return (attn_grad, weight_grad, gain_grad)


def solution(mesh):
    finer = Mesh(mesh.devices.reshape(4, 8, mesh.shape["seq"] // 2, 2), (*DP, *SEQ))
    placed = (
        P(DP, SEQ, None, None),
        P(DP, SEQ, None),
        P(DP, SEQ, None, None, None),
        P(DP, SEQ, None, None, None),
        P(),
        P(),
    )
    return jax.shard_map(
        on_device,
        mesh=finer,
        in_specs=placed,
        out_specs=(P(DP, SEQ, None, None, None), P(DP, None), P()),
        check_vma=False,
    )
```

```python
import functools

import jax
import jax.numpy as jnp
from jax import lax
from jax.experimental import pallas as pl
from jax.experimental.pallas import tpu as pltpu
from jax.sharding import Mesh
from jax.sharding import PartitionSpec as P

DP = ("dp_0", "dp_1", "dp_2")
FIRST = ("dp_0", "dp_2")
SECOND = ("dp_1", "z")
SEQ = ("z", "core")
LANES = 128

epsilon = 1e-06
f32 = jnp.float32
bf16 = jnp.bfloat16
VMEM = pl.BlockSpec(memory_space=pltpu.VMEM)
SMEM = pl.BlockSpec(memory_space=pltpu.SMEM)
FAR = pl.BlockSpec(memory_space=pltpu.HBM)


def call(kernel, name, outs, ins, flops=0, limit=24, far_in=(), far_out=(), scratch=()):
    specs = [SMEM if a.shape == (1,) else (FAR if n in far_in else VMEM) for n, a in enumerate(ins)]
    moved = sum(a.size * a.dtype.itemsize for a in (*ins, *outs))
    return pl.pallas_call(
        kernel,
        name=name,
        out_shape=outs,
        in_specs=specs,
        out_specs=tuple(FAR if n in far_out else VMEM for n in range(len(outs))),
        scratch_shapes=scratch,
        compiler_params=pltpu.CompilerParams(vmem_limit_bytes=limit * 1024 * 1024),
        cost_estimate=pl.CostEstimate(flops=max(flops, 1000000), bytes_accessed=moved, transcendentals=0),
    )(*ins)


def exchange(blocks, axes):
    return lax.all_to_all(blocks, axes, 0, 0, tiled=True)


def iota(shape, dim):
    return lax.broadcasted_iota(jnp.int32, shape, dim)


def gather_kernel(buckets, capacity, patches, chunks, owner_ref, rows_ref, out_ref, hold_ref, sems):
    count = owner_ref.shape[1]
    features = rows_ref.shape[2]
    owner = owner_ref[...]
    picked = (iota((buckets, count), 0) == owner).astype(f32)
    earlier = (iota((count, count), 0) < iota((count, count), 1)).astype(f32)
    before = jnp.dot(picked.astype(bf16), earlier.astype(bf16), preferred_element_type=f32)
    ranking = jnp.sum(before * picked, axis=0, keepdims=True)
    target = owner.astype(f32) * capacity + ranking
    spread = (iota((count, count * patches), 0) == iota((count, count * patches), 1) // patches).astype(bf16)
    wide = jnp.dot(jnp.broadcast_to(target, (8, count)).astype(bf16), spread, preferred_element_type=f32)[:1]
    place = wide.astype(jnp.int32) * patches + iota((1, count * patches), 1) % patches
    lines = rows_ref[...].reshape(count * patches, features)
    step = out_ref.shape[0] // chunks
    copies = []
    for n in range(chunks):
        placing = (iota((step, count * patches), 0) + n * step == place).astype(bf16)
        at = pl.ds(n * step, step)
        hold_ref[at, :] = jnp.dot(placing, lines, preferred_element_type=f32).astype(bf16)
        copies.append(pltpu.make_async_copy(hold_ref.at[at, :], out_ref.at[at, :], sems.at[n]))
        copies[-1].start()
    for copy in copies:
        copy.wait()


def prepare_kernel(step, xact_ref, acts_ref, pair_ref, lines_ref, inverse_ref, left_ref, left_pair_ref):
    slots, patches, features = xact_ref.shape
    height = step * patches
    for n in range(slots // step):
        at = slice(n * height, (n + 1) * height)
        lines = xact_ref[n * step:(n + 1) * step].reshape(height, features)
        lines_ref[at, :] = lines
        values = lines.astype(f32)
        inverse_ref[at, :] = lax.rsqrt(jnp.mean(values * values, axis=1, keepdims=True) + epsilon)
    for source, target in ((acts_ref, left_ref), (pair_ref, left_pair_ref)):
        width = LANES
        for n in range(slots * patches // width):
            block = source[n * width // patches:(n + 1) * width // patches].reshape(width, features)
            target[:, n * width:(n + 1) * width] = block.T


def norm_kernel(
    chunks, step, core_ref, recv_ref, lines_ref, left_ref, left_pair_ref, inverse_ref, gamma_ref,
    keep_ref, send_ref, left_out_ref, left_pair_out_ref, gain_ref, hold_ref, values_ref, sems, left_sems,
):
    rows, features = recv_ref.shape
    half = features // 2
    height = rows // chunks
    first = core_ref[0] == 0
    gamma = gamma_ref[...]
    incoming = []
    for n in range(chunks):
        at = pl.ds(n * height, height)
        incoming.append((
            pltpu.make_async_copy(recv_ref.at[at, :], hold_ref.at[at, :], sems.at[2 * n]),
            pltpu.make_async_copy(lines_ref.at[at, :], values_ref.at[at, :], sems.at[2 * n + 1]),
        ))
        for copy in incoming[-1]:
            copy.start()
    lefts = (
        pltpu.make_async_copy(left_ref, left_out_ref, left_sems.at[0]),
        pltpu.make_async_copy(left_pair_ref, left_pair_out_ref, left_sems.at[1]),
    )
    for copy in lefts:
        copy.start()

    def body(i, gain):
        at = pl.ds(pl.multiple_of(i * step, step), step)
        inverse = inverse_ref[at, :]
        normed = values_ref[at, :].astype(f32) * inverse
        gradient = hold_ref[at, :].astype(f32)
        both = gradient * normed
        gain = gain + both.reshape(step // 8, 8, features).sum(0)
        centre = jnp.mean(gamma * both, axis=1, keepdims=True)
        made = (inverse * (gamma * gradient - normed * centre)).astype(bf16)
        low, high = made[:, :half], made[:, half:]
        keep_ref[at, :] = jnp.where(first, low, high)
        send_ref[at, :] = jnp.where(first, high, low)
        return gain

    gain = jnp.zeros((8, features), f32)
    for n in range(chunks):
        for copy in incoming[n]:
            copy.wait()
        gain = lax.fori_loop(n * height // step, (n + 1) * height // step, body, gain, unroll=2)
    gain_ref[...] = jnp.sum(gain, axis=0, keepdims=True)
    for copy in lefts:
        copy.wait()


def whole_kernel(core_ref, keep_ref, send_ref, grad_ref):
    half = keep_ref.shape[1]
    first = core_ref[0] == 0
    keep, send = keep_ref[...], send_ref[...]
    grad_ref[:, :half] = jnp.where(first, keep, send)
    grad_ref[:, half:] = jnp.where(first, send, keep)


def weight_kernel(shape, left_ref, left_pair_ref, right_ref, right_pair_ref, gain_ref, out_ref):
    outer, middle, inner = shape
    rows = (out_ref.shape[1] - 8) // middle
    width = out_ref.shape[2]
    gain = gain_ref[...]
    chunks = gain.shape[1] // LANES
    for b in range(outer):
        at = slice(b * middle * inner * rows, (b + 1) * middle * inner * rows)
        block = (
            jnp.dot(left_ref[at, :], right_ref[...], preferred_element_type=f32)
            + jnp.dot(left_pair_ref[at, :], right_pair_ref[...], preferred_element_type=f32)
        ).astype(bf16)
        for i in range(inner):
            lines = []
            for m in range(middle):
                own = m * inner + i
                out_ref[b * inner + i, m * rows:(m + 1) * rows, :] = block[own * rows:(own + 1) * rows, :]
                n = b * middle * inner + own
                if n < chunks:
                    lines.append(gain[:, n * LANES:(n + 1) * LANES])
            out_ref[b * inner + i, middle * rows:, :] = jnp.zeros((8, width), bf16)
            if lines:
                lines += [jnp.zeros((1, LANES), f32)] * (8 - len(lines))
                out_ref[b * inner + i, middle * rows:, :LANES] = jnp.concatenate(lines, axis=0).astype(bf16)


def first_sum_kernel(middle, in_ref, out_ref):
    pieces, height, width = out_ref.shape
    pieces //= middle
    rows = (in_ref.shape[1] - 8) // middle
    lines = in_ref[:, middle * rows:, :].astype(f32).sum(0)
    for m in range(middle):
        total = in_ref[:, m * rows:(m + 1) * rows, :].astype(f32).sum(0)
        for p in range(pieces):
            if p * height < rows:
                piece = total[p * height:(p + 1) * height, :]
            elif p * height == rows:
                piece = jnp.where(iota((height, width), 0) == 0, lines[m:m + 1, :], 0.0)
            else:
                piece = jnp.zeros((height, width), f32)
            out_ref[m * pieces + p] = piece.astype(bf16)


def second_sum_kernel(in_ref, out_ref):
    total = in_ref[...].astype(f32).sum(0)
    total = total.astype(bf16)
    for b in range(out_ref.shape[0]):
        out_ref[b] = total


def joined_kernel(in_ref, weight_ref, note_ref):
    pieces, height, half = in_ref.shape
    rows = weight_ref.shape[0]
    squares = jnp.zeros((height, half), f32)
    for p in range(pieces):
        at = (p // 2) * height
        if at < rows:
            block = in_ref[p].astype(f32)
            squares += block * block
            weight_ref[at:at + height, (p % 2) * half:(p % 2 + 1) * half] = block
    p = 2 * (rows // height)
    gain = (in_ref[p].astype(f32) + in_ref[p + 1].astype(f32))[:1, :LANES]
    line = jnp.concatenate([gain, jnp.full((1, LANES), jnp.sum(squares), f32)], axis=1)
    for d in range(note_ref.shape[0]):
        note_ref[d] = line


def scale_kernel(features, note_ref, weight_ref, weight_out_ref, gain_out_ref):
    chunks = features // LANES
    notes = note_ref[...]
    squares = jnp.sum(jnp.max(notes[:, :, LANES:], axis=2))
    gain = notes[:chunks, :, :LANES]
    total = squares + jnp.sum(gain * gain)
    factor = f32(features) * lax.rsqrt(jnp.full((1, LANES), total + epsilon, f32))
    for n in range(chunks):
        gain_out_ref[n * LANES:(n + 1) * LANES] = (gain[n] * factor)[0]
        at = slice(n * LANES, (n + 1) * LANES)
        weight_out_ref[:, at] = weight_ref[:, at] * factor


def on_device(grad_rows, row_owner, acts, xact, gamma, w_out):
    seq_count = lax.axis_size(SEQ)
    outer, middle, inner, z_count = (lax.axis_size(a) for a in (*DP, "z"))
    tokens = row_owner.shape[1]
    slot_count, patches, features = acts.shape[2:]
    capacity = slot_count // seq_count
    rows = slot_count * patches
    half = features // 2
    core = jnp.reshape(lax.axis_index("core"), (1,)).astype(jnp.int32)
    swap = [(0, 1), (1, 0)]

    def shaped(dtype, *shape):
        return jax.ShapeDtypeStruct(shape, dtype)

    chunks = 3
    (outgoing,) = call(
        functools.partial(gather_kernel, seq_count, capacity, patches, chunks),
        "gather_rows",
        (shaped(bf16, rows, features),),
        (row_owner.reshape(1, tokens), grad_rows.reshape(tokens, patches, features)),
        far_out=(0,),
        limit=60,
        scratch=[pltpu.VMEM((rows, features), bf16), pltpu.SemaphoreType.DMA((chunks,))],
    )
    received = exchange(outgoing.reshape(seq_count, capacity * patches, features), SEQ)

    act_slots = acts.reshape(slot_count, patches, features)
    act_pair = lax.ppermute(act_slots, "core", swap)
    lines, inverse, left, left_pair = call(
        functools.partial(prepare_kernel, 8),
        "prepare",
        (
            shaped(bf16, rows, features),
            shaped(f32, rows, 1),
            shaped(bf16, features, rows),
            shaped(bf16, features, rows),
        ),
        (xact.reshape(slot_count, patches, features), act_slots, act_pair),
    )

    chunks = 4
    grad_keep, grad_send, left, left_pair, gain_part = call(
        functools.partial(norm_kernel, chunks, 16),
        "norm_backward",
        (
            shaped(bf16, rows, half),
            shaped(bf16, rows, half),
            shaped(bf16, features, rows),
            shaped(bf16, features, rows),
            shaped(f32, 1, features),
        ),
        (core, received.reshape(rows, features), lines, left, left_pair, inverse, gamma.reshape(1, features)),
        far_in=(1, 2, 3, 4),
        limit=50,
        scratch=[
            pltpu.VMEM((rows, features), bf16),
            pltpu.VMEM((rows, features), bf16),
            pltpu.SemaphoreType.DMA((2 * chunks,)),
            pltpu.SemaphoreType.DMA((2,)),
        ],
    )
    grad_pair = lax.ppermute(grad_send, "core", swap)
    (grad,) = call(
        whole_kernel, "whole_grad", (shaped(bf16, rows, features),), (core, grad_keep, grad_send), limit=52
    )
    grad, grad_keep = lax.optimization_barrier((grad, grad_keep))

    out_rows = features // (outer * middle * inner)
    z_rows = (out_rows + 8) // z_count
    (weight_pair,) = call(
        functools.partial(weight_kernel, (outer, middle, inner)),
        "weight_pair",
        (shaped(bf16, outer * inner, middle * out_rows + 8, half),),
        (left, left_pair, grad_keep, grad_pair, gain_part),
        flops=4 * features * half * rows,
    )
    (weight_some,) = call(
        functools.partial(first_sum_kernel, middle),
        "sum_first",
        (shaped(bf16, middle * z_count, z_rows, half),),
        (exchange(weight_pair, FIRST),),
    )
    (pieces,) = call(
        second_sum_kernel,
        "sum_second",
        (shaped(bf16, seq_count, z_rows, half),),
        (exchange(weight_some, SECOND),),
    )
    weight_sum, note = call(
        joined_kernel,
        "joined",
        (shaped(f32, out_rows, features), shaped(f32, outer * middle * inner, 1, 2 * LANES)),
        (exchange(pieces, SEQ),),
    )
    attn_grad = lax.dot_general(
        grad, w_out, (((1,), (1,)), ((), ())), preferred_element_type=f32
    ).astype(bf16).reshape(acts.shape)
    weight_grad, gain_grad = call(
        functools.partial(scale_kernel, features),
        "scaled",
        (shaped(f32, out_rows, features), shaped(f32, features)),
        (exchange(note, DP), weight_sum),
    )
    return (attn_grad, weight_grad, gain_grad)


def solution(mesh):
    finer = Mesh(mesh.devices.reshape(4, 4, 2, mesh.shape["seq"] // 2, 2), (*DP, *SEQ))
    placed = (
        P(DP, SEQ, None, None),
        P(DP, SEQ, None),
        P(DP, SEQ, None, None, None),
        P(DP, SEQ, None, None, None),
        P(),
        P(),
    )
    return jax.shard_map(
        on_device,
        mesh=finer,
        in_specs=placed,
        out_specs=(P(DP, SEQ, None, None, None), P(DP, None), P()),
        check_vma=False,
    )
```

```python
import functools
import itertools

import jax
import jax.numpy as jnp
from jax import lax
from jax.experimental import pallas as pl
from jax.experimental.pallas import tpu as pltpu
from jax.sharding import Mesh
from jax.sharding import PartitionSpec as P

DP = ("x", "y")
SEQ = ("z", "core")
ALL = (*DP, *SEQ)
LANES = 128

epsilon = 1e-06
f32 = jnp.float32
bf16 = jnp.bfloat16
VMEM = pl.BlockSpec(memory_space=pltpu.VMEM)
SMEM = pl.BlockSpec(memory_space=pltpu.SMEM)
FAR = pl.BlockSpec(memory_space=pltpu.HBM)


def call(kernel, name, outs, ins, flops=0, limit=24, far_in=(), far_out=(), scratch=()):
    specs = [SMEM if a.shape == (1,) else (FAR if n in far_in else VMEM) for n, a in enumerate(ins)]
    moved = sum(a.size * a.dtype.itemsize for a in (*ins, *outs))
    return pl.pallas_call(
        kernel,
        name=name,
        out_shape=outs,
        in_specs=specs,
        out_specs=tuple(FAR if n in far_out else VMEM for n in range(len(outs))),
        scratch_shapes=scratch,
        compiler_params=pltpu.CompilerParams(vmem_limit_bytes=limit * 1024 * 1024),
        cost_estimate=pl.CostEstimate(flops=max(flops, 1000000), bytes_accessed=moved, transcendentals=0),
    )(*ins)


def exchange(blocks, axes, groups=None):
    return lax.all_to_all(blocks, axes, 0, 0, axis_index_groups=groups, tiled=True)


class Cells:
    def __init__(self, counts, core):
        x, y, z = self.counts = counts
        self.core = core
        self.near = list(itertools.product(range(2), repeat=3))
        self.far = list(itertools.product(range(x // 2), range(y // 2), range(z // 2)))
        self.far_xy = list(itertools.product(range(x // 2), range(y // 2)))

    def chip(self, far, near):
        return tuple((2 * f + n + self.core) % c for f, n, c in zip(far, near, self.counts))

    def device(self, far, near):
        x, y, z = self.chip(far, near)
        return ((x * self.counts[1] + y) * self.counts[2] + z) * 2 + self.core

    def inside(self):
        return [[self.device(far, near) for near in self.near] for far in self.far]

    def across(self):
        return [[self.device(far, near) for far in self.far] for near in self.near]

    def replicas(self, near):
        chips = [self.chip((*far, 0), near) for far in self.far_xy]
        return [x * self.counts[1] + y for x, y, _ in chips]

    def order(self):
        return [n * 2 + near[2] for near in self.near for n in self.replicas(near)]

    def gain_rows(self, chunks):
        return [[n if near[2] == 0 and n < chunks else None for n in self.replicas(near)] for near in self.near]


def iota(shape, dim):
    return lax.broadcasted_iota(jnp.int32, shape, dim)


def gather_kernel(buckets, capacity, patches, chunks, owner_ref, rows_ref, out_ref, hold_ref, sems):
    count = owner_ref.shape[1]
    features = rows_ref.shape[2]
    owner = owner_ref[...]
    picked = (iota((buckets, count), 0) == owner).astype(f32)
    earlier = (iota((count, count), 0) < iota((count, count), 1)).astype(f32)
    before = jnp.dot(picked.astype(bf16), earlier.astype(bf16), preferred_element_type=f32)
    ranking = jnp.sum(before * picked, axis=0, keepdims=True)
    target = owner.astype(f32) * capacity + ranking
    spread = (iota((count, count * patches), 0) == iota((count, count * patches), 1) // patches).astype(bf16)
    wide = jnp.dot(jnp.broadcast_to(target, (8, count)).astype(bf16), spread, preferred_element_type=f32)[:1]
    place = wide.astype(jnp.int32) * patches + iota((1, count * patches), 1) % patches
    lines = rows_ref[...].reshape(count * patches, features)
    step = out_ref.shape[0] // chunks
    copies = []
    for n in range(chunks):
        placing = (iota((step, count * patches), 0) + n * step == place).astype(bf16)
        at = pl.ds(n * step, step)
        hold_ref[at, :] = jnp.dot(placing, lines, preferred_element_type=f32).astype(bf16)
        copies.append(pltpu.make_async_copy(hold_ref.at[at, :], out_ref.at[at, :], sems.at[n]))
        copies[-1].start()
    for copy in copies:
        copy.wait()


def in_order(target, lane, turned, order):
    size = turned.shape[0] // len(order)
    for place, first in enumerate(order):
        rows = turned[first * size:(first + 1) * size]
        target[place * size:(place + 1) * size, lane:lane + turned.shape[1]] = rows


def prepare_kernel(step, orders, core_ref, xact_ref, acts_ref, pair_ref, lines_ref, inverse_ref, left_ref, left_pair_ref):
    slots, patches, features = xact_ref.shape
    height = step * patches
    for n in range(slots // step):
        at = slice(n * height, (n + 1) * height)
        lines = xact_ref[n * step:(n + 1) * step].reshape(height, features)
        lines_ref[at, :] = lines
        values = lines.astype(f32)
        inverse_ref[at, :] = lax.rsqrt(jnp.mean(values * values, axis=1, keepdims=True) + epsilon)
    for source, target in ((acts_ref, left_ref), (pair_ref, left_pair_ref)):
        width = LANES
        for n in range(slots * patches // width):
            block = source[n * width // patches:(n + 1) * width // patches].reshape(width, features)
            turned = block.T
            for core, order in enumerate(orders):
                pl.when(core_ref[0] == core)(functools.partial(in_order, target, n * width, turned, order))


def norm_kernel(
    chunks, step, core_ref, recv_ref, lines_ref, left_ref, left_pair_ref, far_ref, gamma_ref,
    keep_ref, send_ref, left_out_ref, left_pair_out_ref, gain_ref, hold_ref, values_ref, inverse_ref, sems, left_sems,
):
    rows, features = recv_ref.shape
    half = features // 2
    height = rows // chunks
    first = core_ref[0] == 0
    gamma = gamma_ref[...]
    scales = pltpu.make_async_copy(far_ref, inverse_ref, left_sems.at[2])
    scales.start()
    incoming = []
    for n in range(chunks):
        at = pl.ds(n * height, height)
        incoming.append((
            pltpu.make_async_copy(recv_ref.at[at, :], hold_ref.at[at, :], sems.at[2 * n]),
            pltpu.make_async_copy(lines_ref.at[at, :], values_ref.at[at, :], sems.at[2 * n + 1]),
        ))
        for copy in incoming[-1]:
            copy.start()
    lefts = (
        pltpu.make_async_copy(left_ref, left_out_ref, left_sems.at[0]),
        pltpu.make_async_copy(left_pair_ref, left_pair_out_ref, left_sems.at[1]),
    )
    for copy in lefts:
        copy.start()

    def body(i, gain):
        at = pl.ds(pl.multiple_of(i * step, step), step)
        inverse = inverse_ref[at, :]
        normed = values_ref[at, :].astype(f32) * inverse
        gradient = hold_ref[at, :].astype(f32)
        both = gradient * normed
        gain = gain + both.reshape(step // 8, 8, features).sum(0)
        centre = jnp.mean(gamma * both, axis=1, keepdims=True)
        made = (inverse * (gamma * gradient - normed * centre)).astype(bf16)
        low, high = made[:, :half], made[:, half:]
        keep_ref[at, :] = jnp.where(first, low, high)
        send_ref[at, :] = jnp.where(first, high, low)
        return gain

    gain = jnp.zeros((8, features), f32)
    scales.wait()
    for n in range(chunks):
        for copy in incoming[n]:
            copy.wait()
        gain = lax.fori_loop(n * height // step, (n + 1) * height // step, body, gain, unroll=3)
    gain_ref[...] = jnp.sum(gain, axis=0, keepdims=True)
    for copy in lefts:
        copy.wait()


def whole_kernel(core_ref, keep_ref, send_ref, grad_ref):
    half = keep_ref.shape[1]
    first = core_ref[0] == 0
    keep, send = keep_ref[...], send_ref[...]
    grad_ref[:, :half] = jnp.where(first, keep, send)
    grad_ref[:, half:] = jnp.where(first, send, keep)


def gain_tiles(gain_rows, gain, out_ref):
    rows = out_ref.shape[1] - 8
    for b, numbers in enumerate(gain_rows):
        if any(n is not None for n in numbers):
            lines = [
                jnp.zeros((1, LANES), f32) if n is None else gain[:, n * LANES:(n + 1) * LANES] for n in numbers
            ]
            lines += [jnp.zeros((1, LANES), f32)] * (8 - len(lines))
            out_ref[b, rows:, :LANES] = jnp.concatenate(lines, axis=0).astype(bf16)


def weight_kernel(gain_rows, core_ref, left_ref, left_pair_ref, right_ref, right_pair_ref, gain_ref, out_ref):
    blocks, height, width = out_ref.shape
    rows = height - 8
    gain = gain_ref[...]
    for b in range(blocks):
        at = slice(b * rows, (b + 1) * rows)
        out_ref[b, :rows, :] = (
            jnp.dot(left_ref[at, :], right_ref[...], preferred_element_type=f32)
            + jnp.dot(left_pair_ref[at, :], right_pair_ref[...], preferred_element_type=f32)
        ).astype(bf16)
        out_ref[b, rows:, :] = jnp.zeros((8, width), bf16)
    for core, numbers in enumerate(gain_rows):
        pl.when(core_ref[0] == core)(functools.partial(gain_tiles, numbers, gain, out_ref))


def first_sum_kernel(middle, in_ref, out_ref):
    pieces, height, width = out_ref.shape
    pieces //= middle
    rows = (in_ref.shape[1] - 8) // middle
    total = in_ref[...].astype(f32).sum(0)
    for m in range(middle):
        for p in range(pieces):
            if p * height < rows:
                piece = total[m * rows + p * height:m * rows + (p + 1) * height, :]
            elif p * height == rows:
                piece = jnp.where(iota((height, width), 0) == 0, total[middle * rows + m:middle * rows + m + 1, :], 0.0)
            else:
                piece = jnp.zeros((height, width), f32)
            out_ref[m * pieces + p] = piece.astype(bf16)


def second_sum_kernel(in_ref, out_ref):
    total = in_ref[...].astype(f32).sum(0)
    total = total.astype(bf16)
    for b in range(out_ref.shape[0]):
        out_ref[b] = total


def joined_kernel(in_ref, weight_ref, note_ref):
    pieces, height, half = in_ref.shape
    part = weight_ref.shape[0] // 2
    squares = jnp.zeros((height, half), f32)
    gain = jnp.zeros((1, LANES), f32)
    for p in range(pieces):
        core = p % 2
        far, near = divmod((p // 2 - core) % (pieces // 2), 2)
        block = in_ref[p].astype(f32)
        if far * height < part:
            at = near * part + far * height
            squares += block * block
            weight_ref[at:at + height, core * half:(core + 1) * half] = block
        elif near == 0:
            gain += block[:1, :LANES]
    line = jnp.concatenate([gain, jnp.full((1, LANES), jnp.sum(squares), f32)], axis=1)
    for d in range(note_ref.shape[0]):
        note_ref[d] = line


def scale_kernel(features, note_ref, weight_ref, weight_out_ref, gain_out_ref):
    chunks = features // LANES
    notes = note_ref[...]
    squares = jnp.sum(jnp.max(notes[:, :, LANES:], axis=2))
    gain = notes[:chunks, :, :LANES]
    total = squares + jnp.sum(gain * gain)
    factor = f32(features) * lax.rsqrt(jnp.full((1, LANES), total + epsilon, f32))
    for n in range(chunks):
        gain_out_ref[n * LANES:(n + 1) * LANES] = (gain[n] * factor)[0]
        at = slice(n * LANES, (n + 1) * LANES)
        weight_out_ref[:, at] = weight_ref[:, at] * factor


def on_device(grad_rows, row_owner, acts, xact, gamma, w_out):
    seq_count = lax.axis_size(SEQ)
    counts = tuple(lax.axis_size(a) for a in (*DP, SEQ[0]))
    cells = [Cells(counts, core) for core in range(2)]
    inside = [group for c in cells for group in c.inside()]
    across = [group for c in cells for group in c.across()]
    tokens = row_owner.shape[1]
    slot_count, patches, features = acts.shape[2:]
    capacity = slot_count // seq_count
    rows = slot_count * patches
    half = features // 2
    core = jnp.reshape(lax.axis_index("core"), (1,)).astype(jnp.int32)
    swap = [(0, 1), (1, 0)]

    def shaped(dtype, *shape):
        return jax.ShapeDtypeStruct(shape, dtype)

    chunks = 3
    (outgoing,) = call(
        functools.partial(gather_kernel, seq_count, capacity, patches, chunks),
        "gather_rows",
        (shaped(bf16, rows, features),),
        (row_owner.reshape(1, tokens), grad_rows.reshape(tokens, patches, features)),
        far_out=(0,),
        limit=60,
        scratch=[pltpu.VMEM((rows, features), bf16), pltpu.SemaphoreType.DMA((chunks,))],
    )
    received = exchange(outgoing.reshape(seq_count, capacity * patches, features), SEQ)

    act_slots = acts.reshape(slot_count, patches, features)
    act_pair = lax.ppermute(act_slots, "core", swap)
    lines, inverse, left, left_pair = call(
        functools.partial(prepare_kernel, 8, [c.order() for c in cells]),
        "prepare",
        (
            shaped(bf16, rows, features),
            shaped(f32, rows, 1),
            shaped(bf16, features, rows),
            shaped(bf16, features, rows),
        ),
        (core, xact.reshape(slot_count, patches, features), act_slots, act_pair),
    )

    chunks = 8
    grad_keep, grad_send, left, left_pair, gain_part = call(
        functools.partial(norm_kernel, chunks, 16),
        "norm_backward",
        (
            shaped(bf16, rows, half),
            shaped(bf16, rows, half),
            shaped(bf16, features, rows),
            shaped(bf16, features, rows),
            shaped(f32, 1, features),
        ),
        (core, received.reshape(rows, features), lines, left, left_pair, inverse, gamma.reshape(1, features)),
        far_in=(1, 2, 3, 4, 5),
        limit=50,
        scratch=[
            pltpu.VMEM((rows, features), bf16),
            pltpu.VMEM((rows, features), bf16),
            pltpu.VMEM((rows, 1), f32),
            pltpu.SemaphoreType.DMA((2 * chunks,)),
            pltpu.SemaphoreType.DMA((3,)),
        ],
    )
    grad_pair = lax.ppermute(grad_send, "core", swap)
    (grad,) = call(
        whole_kernel, "whole_grad", (shaped(bf16, rows, features),), (core, grad_keep, grad_send), limit=52
    )
    grad, grad_keep = lax.optimization_barrier((grad, grad_keep))

    replicas = counts[0] * counts[1]
    out_rows = features // replicas
    z_rows = out_rows // 2 // (counts[2] // 2 - 1)
    (weight_pair,) = call(
        functools.partial(weight_kernel, [c.gain_rows(features // LANES) for c in cells]),
        "weight_pair",
        (shaped(bf16, 8, features // 8 + 8, half),),
        (core, left, left_pair, grad_keep, grad_pair, gain_part),
        flops=4 * features * half * rows,
    )
    (weight_some,) = call(
        functools.partial(first_sum_kernel, replicas // 4),
        "sum_first",
        (shaped(bf16, replicas // 4 * counts[2] // 2, z_rows, half),),
        (exchange(weight_pair, ALL, inside),),
    )
    (pieces,) = call(
        second_sum_kernel,
        "sum_second",
        (shaped(bf16, seq_count, z_rows, half),),
        (exchange(weight_some, ALL, across),),
    )
    weight_sum, note = call(
        joined_kernel,
        "joined",
        (shaped(f32, out_rows, features), shaped(f32, replicas, 1, 2 * LANES)),
        (exchange(pieces, SEQ),),
    )
    attn_grad = lax.dot_general(
        grad, w_out, (((1,), (1,)), ((), ())), preferred_element_type=f32
    ).astype(bf16).reshape(acts.shape)
    weight_grad, gain_grad = call(
        functools.partial(scale_kernel, features),
        "scaled",
        (shaped(f32, out_rows, features), shaped(f32, features)),
        (exchange(note, DP), weight_sum),
    )
    return (attn_grad, weight_grad, gain_grad)


def solution(mesh):
    finer = Mesh(mesh.devices.reshape(4, 8, mesh.shape["seq"] // 2, 2), ALL)
    placed = (
        P(DP, SEQ, None, None),
        P(DP, SEQ, None),
        P(DP, SEQ, None, None, None),
        P(DP, SEQ, None, None, None),
        P(),
        P(),
    )
    return jax.shard_map(
        on_device,
        mesh=finer,
        in_specs=placed,
        out_specs=(P(DP, SEQ, None, None, None), P(DP, None), P()),
        check_vma=False,
    )
```

```python
import functools
import itertools

import jax
import jax.numpy as jnp
from jax import lax
from jax.experimental import pallas as pl
from jax.experimental.pallas import tpu as pltpu
from jax.sharding import Mesh
from jax.sharding import PartitionSpec as P

DP = ("x", "y")
SEQ = ("z", "core")
ALL = (*DP, *SEQ)
LANES = 128

epsilon = 1e-06
f32 = jnp.float32
bf16 = jnp.bfloat16
VMEM = pl.BlockSpec(memory_space=pltpu.VMEM)
SMEM = pl.BlockSpec(memory_space=pltpu.SMEM)
FAR = pl.BlockSpec(memory_space=pltpu.HBM)


def call(kernel, name, outs, ins, flops=0, limit=24, far_in=(), far_out=(), scratch=()):
    specs = [SMEM if a.shape == (1,) else (FAR if n in far_in else VMEM) for n, a in enumerate(ins)]
    moved = sum(a.size * a.dtype.itemsize for a in (*ins, *outs))
    return pl.pallas_call(
        kernel,
        name=name,
        out_shape=outs,
        in_specs=specs,
        out_specs=tuple(FAR if n in far_out else VMEM for n in range(len(outs))),
        scratch_shapes=scratch,
        compiler_params=pltpu.CompilerParams(vmem_limit_bytes=limit * 1024 * 1024),
        cost_estimate=pl.CostEstimate(flops=max(flops, 1000000), bytes_accessed=moved, transcendentals=0),
    )(*ins)


def exchange(blocks, axes, groups=None):
    return lax.all_to_all(blocks, axes, 0, 0, axis_index_groups=groups, tiled=True)


class Cells:
    def __init__(self, counts, core):
        x, y, z = self.counts = counts
        self.core = core
        self.near = list(itertools.product(range(2), repeat=3))
        self.far = list(itertools.product(range(x // 2), range(y // 2), range(z // 2)))
        self.far_xy = list(itertools.product(range(x // 2), range(y // 2)))

    def chip(self, far, near):
        return tuple((2 * f + n + self.core) % c for f, n, c in zip(far, near, self.counts))

    def device(self, far, near):
        x, y, z = self.chip(far, near)
        return ((x * self.counts[1] + y) * self.counts[2] + z) * 2 + self.core

    def inside(self):
        return [[self.device(far, near) for near in self.near] for far in self.far]

    def across(self):
        return [[self.device(far, near) for far in self.far] for near in self.near]

    def replicas(self, near):
        chips = [self.chip((*far, 0), near) for far in self.far_xy]
        return [x * self.counts[1] + y for x, y, _ in chips]

    def order(self):
        return [n * 2 + near[2] for near in self.near for n in self.replicas(near)]

    def gain_rows(self, chunks):
        return [[n if near[2] == 0 and n < chunks else None for n in self.replicas(near)] for near in self.near]


def iota(shape, dim):
    return lax.broadcasted_iota(jnp.int32, shape, dim)


def gather_kernel(buckets, capacity, patches, chunks, owner_ref, rows_ref, out_ref, hold_ref, sems):
    count = owner_ref.shape[1]
    features = rows_ref.shape[2]
    owner = owner_ref[...]
    picked = (iota((buckets, count), 0) == owner).astype(f32)
    earlier = (iota((count, count), 0) < iota((count, count), 1)).astype(f32)
    before = jnp.dot(picked.astype(bf16), earlier.astype(bf16), preferred_element_type=f32)
    ranking = jnp.sum(before * picked, axis=0, keepdims=True)
    target = owner.astype(f32) * capacity + ranking
    spread = (iota((count, count * patches), 0) == iota((count, count * patches), 1) // patches).astype(bf16)
    wide = jnp.dot(jnp.broadcast_to(target, (8, count)).astype(bf16), spread, preferred_element_type=f32)[:1]
    place = wide.astype(jnp.int32) * patches + iota((1, count * patches), 1) % patches
    lines = rows_ref[...].reshape(count * patches, features)
    step = out_ref.shape[0] // chunks
    copies = []
    for n in range(chunks):
        placing = (iota((step, count * patches), 0) + n * step == place).astype(bf16)
        at = pl.ds(n * step, step)
        hold_ref[at, :] = jnp.dot(placing, lines, preferred_element_type=f32).astype(bf16)
        copies.append(pltpu.make_async_copy(hold_ref.at[at, :], out_ref.at[at, :], sems.at[n]))
        copies[-1].start()
    for copy in copies:
        copy.wait()


def in_order(target, lane, turned, order):
    size = turned.shape[0] // len(order)
    for place, first in enumerate(order):
        rows = turned[first * size:(first + 1) * size]
        target[place * size:(place + 1) * size, lane:lane + turned.shape[1]] = rows


def prepare_kernel(step, orders, core_ref, xact_ref, acts_ref, pair_ref, lines_ref, inverse_ref, left_ref, left_pair_ref):
    slots, patches, features = xact_ref.shape
    height = step * patches
    for n in range(slots // step):
        at = slice(n * height, (n + 1) * height)
        lines = xact_ref[n * step:(n + 1) * step].reshape(height, features)
        lines_ref[at, :] = lines
        values = lines.astype(f32)
        inverse_ref[at, :] = lax.rsqrt(jnp.mean(values * values, axis=1, keepdims=True) + epsilon)
    for source, target in ((acts_ref, left_ref), (pair_ref, left_pair_ref)):
        width = LANES
        for n in range(slots * patches // width):
            block = source[n * width // patches:(n + 1) * width // patches].reshape(width, features)
            turned = block.T
            for core, order in enumerate(orders):
                pl.when(core_ref[0] == core)(functools.partial(in_order, target, n * width, turned, order))


def norm_kernel(
    chunks, step, core_ref, recv_ref, lines_ref, left_ref, left_pair_ref, far_ref, gamma_ref,
    keep_ref, send_ref, left_out_ref, left_pair_out_ref, gain_ref, hold_ref, values_ref, inverse_ref, sems, left_sems,
):
    rows, features = recv_ref.shape
    half = features // 2
    height = rows // chunks
    first = core_ref[0] == 0
    gamma = gamma_ref[...]
    scales = pltpu.make_async_copy(far_ref, inverse_ref, left_sems.at[2])
    scales.start()
    incoming = []
    for n in range(chunks):
        at = pl.ds(n * height, height)
        incoming.append((
            pltpu.make_async_copy(recv_ref.at[at, :], hold_ref.at[at, :], sems.at[2 * n]),
            pltpu.make_async_copy(lines_ref.at[at, :], values_ref.at[at, :], sems.at[2 * n + 1]),
        ))
        for copy in incoming[-1]:
            copy.start()
    lefts = (
        pltpu.make_async_copy(left_ref, left_out_ref, left_sems.at[0]),
        pltpu.make_async_copy(left_pair_ref, left_pair_out_ref, left_sems.at[1]),
    )
    for copy in lefts:
        copy.start()

    def body(i, gain):
        at = pl.ds(pl.multiple_of(i * step, step), step)
        inverse = inverse_ref[at, :]
        normed = values_ref[at, :].astype(f32) * inverse
        gradient = hold_ref[at, :].astype(f32)
        both = gradient * normed
        gain = gain + both.reshape(step // 8, 8, features).sum(0)
        centre = jnp.mean(gamma * both, axis=1, keepdims=True)
        made = (inverse * (gamma * gradient - normed * centre)).astype(bf16)
        low, high = made[:, :half], made[:, half:]
        keep_ref[at, :] = jnp.where(first, low, high)
        send_ref[at, :] = jnp.where(first, high, low)
        return gain

    gain = jnp.zeros((8, features), f32)
    scales.wait()
    for n in range(chunks):
        for copy in incoming[n]:
            copy.wait()
        gain = lax.fori_loop(n * height // step, (n + 1) * height // step, body, gain, unroll=3)
    gain_ref[...] = jnp.sum(gain, axis=0, keepdims=True)
    for copy in lefts:
        copy.wait()


def whole_kernel(core_ref, keep_ref, send_ref, grad_ref):
    half = keep_ref.shape[1]
    first = core_ref[0] == 0
    keep, send = keep_ref[...], send_ref[...]
    grad_ref[:, :half] = jnp.where(first, keep, send)
    grad_ref[:, half:] = jnp.where(first, send, keep)


def gain_tiles(gain_rows, gain, out_ref):
    rows = out_ref.shape[1] - 8
    for b, numbers in enumerate(gain_rows):
        if any(n is not None for n in numbers):
            lines = [
                jnp.zeros((1, LANES), f32) if n is None else gain[:, n * LANES:(n + 1) * LANES] for n in numbers
            ]
            lines += [jnp.zeros((1, LANES), f32)] * (8 - len(lines))
            out_ref[b, rows:, :LANES] = jnp.concatenate(lines, axis=0).astype(bf16)


def own_kernel(left_ref, right_ref, out_ref):
    out_ref[...] = jnp.dot(left_ref[...], right_ref[...], preferred_element_type=f32)


def weight_kernel(gain_rows, core_ref, own_ref, left_pair_ref, right_pair_ref, gain_ref, out_ref):
    blocks, height, width = out_ref.shape
    rows = height - 8
    gain = gain_ref[...]
    for b in range(blocks):
        at = slice(b * rows, (b + 1) * rows)
        out_ref[b, :rows, :] = (
            own_ref[at, :]
            + jnp.dot(left_pair_ref[at, :], right_pair_ref[...], preferred_element_type=f32)
        ).astype(bf16)
        out_ref[b, rows:, :] = jnp.zeros((8, width), bf16)
    for core, numbers in enumerate(gain_rows):
        pl.when(core_ref[0] == core)(functools.partial(gain_tiles, numbers, gain, out_ref))


def first_sum_kernel(middle, in_ref, out_ref):
    pieces, height, width = out_ref.shape
    pieces //= middle
    rows = (in_ref.shape[1] - 8) // middle
    total = in_ref[...].astype(f32).sum(0)
    for m in range(middle):
        for p in range(pieces):
            if p * height < rows:
                piece = total[m * rows + p * height:m * rows + (p + 1) * height, :]
            elif p * height == rows:
                piece = jnp.where(iota((height, width), 0) == 0, total[middle * rows + m:middle * rows + m + 1, :], 0.0)
            else:
                piece = jnp.zeros((height, width), f32)
            out_ref[m * pieces + p] = piece.astype(bf16)


def second_sum_kernel(in_ref, out_ref):
    total = in_ref[...].astype(f32).sum(0)
    total = total.astype(bf16)
    for b in range(out_ref.shape[0]):
        out_ref[b] = total


def joined_kernel(in_ref, weight_ref, note_ref):
    pieces, height, half = in_ref.shape
    part = weight_ref.shape[0] // 2
    squares = jnp.zeros((height, half), f32)
    gain = jnp.zeros((1, LANES), f32)
    for p in range(pieces):
        core = p % 2
        far, near = divmod((p // 2 - core) % (pieces // 2), 2)
        block = in_ref[p].astype(f32)
        if far * height < part:
            at = near * part + far * height
            squares += block * block
            weight_ref[at:at + height, core * half:(core + 1) * half] = block
        elif near == 0:
            gain += block[:1, :LANES]
    line = jnp.concatenate([gain, jnp.full((1, LANES), jnp.sum(squares), f32)], axis=1)
    for d in range(note_ref.shape[0]):
        note_ref[d] = line


def scale_kernel(features, note_ref, weight_ref, weight_out_ref, gain_out_ref):
    chunks = features // LANES
    notes = note_ref[...]
    squares = jnp.sum(jnp.max(notes[:, :, LANES:], axis=2))
    gain = notes[:chunks, :, :LANES]
    total = squares + jnp.sum(gain * gain)
    factor = f32(features) * lax.rsqrt(jnp.full((1, LANES), total + epsilon, f32))
    for n in range(chunks):
        gain_out_ref[n * LANES:(n + 1) * LANES] = (gain[n] * factor)[0]
        at = slice(n * LANES, (n + 1) * LANES)
        weight_out_ref[:, at] = weight_ref[:, at] * factor


def on_device(grad_rows, row_owner, acts, xact, gamma, w_out):
    seq_count = lax.axis_size(SEQ)
    counts = tuple(lax.axis_size(a) for a in (*DP, SEQ[0]))
    cells = [Cells(counts, core) for core in range(2)]
    inside = [group for c in cells for group in c.inside()]
    across = [group for c in cells for group in c.across()]
    tokens = row_owner.shape[1]
    slot_count, patches, features = acts.shape[2:]
    capacity = slot_count // seq_count
    rows = slot_count * patches
    half = features // 2
    core = jnp.reshape(lax.axis_index("core"), (1,)).astype(jnp.int32)
    swap = [(0, 1), (1, 0)]

    def shaped(dtype, *shape):
        return jax.ShapeDtypeStruct(shape, dtype)

    chunks = 3
    (outgoing,) = call(
        functools.partial(gather_kernel, seq_count, capacity, patches, chunks),
        "gather_rows",
        (shaped(bf16, rows, features),),
        (row_owner.reshape(1, tokens), grad_rows.reshape(tokens, patches, features)),
        far_out=(0,),
        limit=60,
        scratch=[pltpu.VMEM((rows, features), bf16), pltpu.SemaphoreType.DMA((chunks,))],
    )
    received = exchange(outgoing.reshape(seq_count, capacity * patches, features), SEQ)

    act_slots = acts.reshape(slot_count, patches, features)
    act_pair = lax.ppermute(act_slots, "core", swap)
    lines, inverse, left, left_pair = call(
        functools.partial(prepare_kernel, 8, [c.order() for c in cells]),
        "prepare",
        (
            shaped(bf16, rows, features),
            shaped(f32, rows, 1),
            shaped(bf16, features, rows),
            shaped(bf16, features, rows),
        ),
        (core, xact.reshape(slot_count, patches, features), act_slots, act_pair),
    )

    chunks = 8
    grad_keep, grad_send, left, left_pair, gain_part = call(
        functools.partial(norm_kernel, chunks, 16),
        "norm_backward",
        (
            shaped(bf16, rows, half),
            shaped(bf16, rows, half),
            shaped(bf16, features, rows),
            shaped(bf16, features, rows),
            shaped(f32, 1, features),
        ),
        (core, received.reshape(rows, features), lines, left, left_pair, inverse, gamma.reshape(1, features)),
        far_in=(1, 2, 3, 4, 5),
        limit=50,
        scratch=[
            pltpu.VMEM((rows, features), bf16),
            pltpu.VMEM((rows, features), bf16),
            pltpu.VMEM((rows, 1), f32),
            pltpu.SemaphoreType.DMA((2 * chunks,)),
            pltpu.SemaphoreType.DMA((3,)),
        ],
    )
    grad_pair = lax.ppermute(grad_send, "core", swap)
    (grad,) = call(
        whole_kernel, "whole_grad", (shaped(bf16, rows, features),), (core, grad_keep, grad_send), limit=52
    )
    (own,) = call(own_kernel, "weight_own", (shaped(f32, features, half),), (left, grad_keep), flops=2 * features * half * rows, limit=20)
    grad, own = lax.optimization_barrier((grad, own))

    replicas = counts[0] * counts[1]
    out_rows = features // replicas
    z_rows = out_rows // 2 // (counts[2] // 2 - 1)
    (weight_pair,) = call(
        functools.partial(weight_kernel, [c.gain_rows(features // LANES) for c in cells]),
        "weight_pair",
        (shaped(bf16, 8, features // 8 + 8, half),),
        (core, own, left_pair, grad_pair, gain_part),
        flops=4 * features * half * rows,
    )
    (weight_some,) = call(
        functools.partial(first_sum_kernel, replicas // 4),
        "sum_first",
        (shaped(bf16, replicas // 4 * counts[2] // 2, z_rows, half),),
        (exchange(weight_pair, ALL, inside),),
    )
    (pieces,) = call(
        second_sum_kernel,
        "sum_second",
        (shaped(bf16, seq_count, z_rows, half),),
        (exchange(weight_some, ALL, across),),
    )
    weight_sum, note = call(
        joined_kernel,
        "joined",
        (shaped(f32, out_rows, features), shaped(f32, replicas, 1, 2 * LANES)),
        (exchange(pieces, SEQ),),
    )
    attn_grad = lax.dot_general(
        grad, w_out, (((1,), (1,)), ((), ())), preferred_element_type=f32
    ).astype(bf16).reshape(acts.shape)
    weight_grad, gain_grad = call(
        functools.partial(scale_kernel, features),
        "scaled",
        (shaped(f32, out_rows, features), shaped(f32, features)),
        (exchange(note, DP), weight_sum),
    )
    return (attn_grad, weight_grad, gain_grad)


def solution(mesh):
    finer = Mesh(mesh.devices.reshape(4, 8, mesh.shape["seq"] // 2, 2), ALL)
    placed = (
        P(DP, SEQ, None, None),
        P(DP, SEQ, None),
        P(DP, SEQ, None, None, None),
        P(DP, SEQ, None, None, None),
        P(),
        P(),
    )
    return jax.shard_map(
        on_device,
        mesh=finer,
        in_specs=placed,
        out_specs=(P(DP, SEQ, None, None, None), P(DP, None), P()),
        check_vma=False,
    )
```

```python
import functools
import itertools

import jax
import jax.numpy as jnp
from jax import lax
from jax.experimental import pallas as pl
from jax.experimental.pallas import tpu as pltpu
from jax.sharding import Mesh
from jax.sharding import PartitionSpec as P

DP = ("x", "y")
SEQ = ("z", "core")
ALL = (*DP, *SEQ)
LANES = 128

epsilon = 1e-06
f32 = jnp.float32
bf16 = jnp.bfloat16
VMEM = pl.BlockSpec(memory_space=pltpu.VMEM)
SMEM = pl.BlockSpec(memory_space=pltpu.SMEM)
FAR = pl.BlockSpec(memory_space=pltpu.HBM)


def call(kernel, name, outs, ins, flops=0, limit=24, far_in=(), far_out=(), scratch=()):
    specs = [SMEM if a.shape == (1,) else (FAR if n in far_in else VMEM) for n, a in enumerate(ins)]
    moved = sum(a.size * a.dtype.itemsize for a in (*ins, *outs))
    return pl.pallas_call(
        kernel,
        name=name,
        out_shape=outs,
        in_specs=specs,
        out_specs=tuple(FAR if n in far_out else VMEM for n in range(len(outs))),
        scratch_shapes=scratch,
        compiler_params=pltpu.CompilerParams(vmem_limit_bytes=int(limit * 1024 * 1024)),
        cost_estimate=pl.CostEstimate(flops=max(flops, 1000000), bytes_accessed=moved, transcendentals=0),
    )(*ins)


def exchange(blocks, axes, groups=None):
    return lax.all_to_all(blocks, axes, 0, 0, axis_index_groups=groups, tiled=True)


class Cells:
    def __init__(self, counts, core):
        x, y, z = self.counts = counts
        self.core = core
        self.near = list(itertools.product(range(2), repeat=3))
        self.far = list(itertools.product(range(x // 2), range(y // 2), range(z // 2)))
        self.far_xy = list(itertools.product(range(x // 2), range(y // 2)))

    def chip(self, far, near):
        return tuple((2 * f + n + self.core) % c for f, n, c in zip(far, near, self.counts))

    def device(self, far, near):
        x, y, z = self.chip(far, near)
        return ((x * self.counts[1] + y) * self.counts[2] + z) * 2 + self.core

    def inside(self):
        return [[self.device(far, near) for near in self.near] for far in self.far]

    def across(self):
        return [[self.device(far, near) for far in self.far] for near in self.near]

    def replicas(self, near):
        chips = [self.chip((*far, 0), near) for far in self.far_xy]
        return [x * self.counts[1] + y for x, y, _ in chips]

    def order(self):
        return [n * 2 + near[2] for near in self.near for n in self.replicas(near)]

    def gain_rows(self, chunks):
        return [[n if near[2] == 0 and n < chunks else None for n in self.replicas(near)] for near in self.near]


def iota(shape, dim):
    return lax.broadcasted_iota(jnp.int32, shape, dim)


def gather_kernel(buckets, capacity, patches, chunks, owner_ref, rows_ref, out_ref, hold_ref, sems):
    count = owner_ref.shape[1]
    features = rows_ref.shape[2]
    owner = owner_ref[...]
    picked = (iota((buckets, count), 0) == owner).astype(f32)
    earlier = (iota((count, count), 0) < iota((count, count), 1)).astype(f32)
    before = jnp.dot(picked.astype(bf16), earlier.astype(bf16), preferred_element_type=f32)
    ranking = jnp.sum(before * picked, axis=0, keepdims=True)
    target = owner.astype(f32) * capacity + ranking
    spread = (iota((count, count * patches), 0) == iota((count, count * patches), 1) // patches).astype(bf16)
    wide = jnp.dot(jnp.broadcast_to(target, (8, count)).astype(bf16), spread, preferred_element_type=f32)[:1]
    place = wide.astype(jnp.int32) * patches + iota((1, count * patches), 1) % patches
    lines = rows_ref[...].reshape(count * patches, features)
    step = out_ref.shape[0] // chunks
    copies = []
    for n in range(chunks):
        placing = (iota((step, count * patches), 0) + n * step == place).astype(bf16)
        at = pl.ds(n * step, step)
        hold_ref[at, :] = jnp.dot(placing, lines, preferred_element_type=f32).astype(bf16)
        copies.append(pltpu.make_async_copy(hold_ref.at[at, :], out_ref.at[at, :], sems.at[n]))
        copies[-1].start()
    for copy in copies:
        copy.wait()


def in_order(target, lane, turned, order):
    size = turned.shape[0] // len(order)
    for place, first in enumerate(order):
        rows = turned[first * size:(first + 1) * size]
        target[place * size:(place + 1) * size, lane:lane + turned.shape[1]] = rows


def prepare_kernel(step, orders, core_ref, xact_ref, acts_ref, pair_ref, lines_ref, inverse_ref, left_ref, left_pair_ref):
    slots, patches, features = xact_ref.shape
    height = step * patches
    for n in range(slots // step):
        at = slice(n * height, (n + 1) * height)
        lines = xact_ref[n * step:(n + 1) * step].reshape(height, features)
        lines_ref[at, :] = lines
        values = lines.astype(f32)
        inverse_ref[at, :] = lax.rsqrt(jnp.mean(values * values, axis=1, keepdims=True) + epsilon)
    for source, target in ((acts_ref, left_ref), (pair_ref, left_pair_ref)):
        width = LANES
        for n in range(slots * patches // width):
            block = source[n * width // patches:(n + 1) * width // patches].reshape(width, features)
            turned = block.T
            for core, order in enumerate(orders):
                pl.when(core_ref[0] == core)(functools.partial(in_order, target, n * width, turned, order))


def norm_kernel(
    chunks, step, core_ref, recv_ref, lines_ref, left_ref, far_ref, gamma_ref,
    keep_ref, send_ref, left_out_ref, gain_ref, hold_ref, values_ref, inverse_ref, sems, left_sems,
):
    rows, features = recv_ref.shape
    half = features // 2
    height = rows // chunks
    first = core_ref[0] == 0
    gamma = gamma_ref[...]
    scales = pltpu.make_async_copy(far_ref, inverse_ref, left_sems.at[1])
    scales.start()
    incoming = []
    for n in range(chunks):
        at = pl.ds(n * height, height)
        incoming.append((
            pltpu.make_async_copy(recv_ref.at[at, :], hold_ref.at[at, :], sems.at[2 * n]),
            pltpu.make_async_copy(lines_ref.at[at, :], values_ref.at[at, :], sems.at[2 * n + 1]),
        ))
        for copy in incoming[-1]:
            copy.start()
    carried = pltpu.make_async_copy(left_ref, left_out_ref, left_sems.at[0])
    carried.start()

    def body(i, gain):
        at = pl.ds(pl.multiple_of(i * step, step), step)
        inverse = inverse_ref[at, :]
        normed = values_ref[at, :].astype(f32) * inverse
        gradient = hold_ref[at, :].astype(f32)
        both = gradient * normed
        gain = gain + both.reshape(step // 8, 8, features).sum(0)
        centre = jnp.mean(gamma * both, axis=1, keepdims=True)
        made = (inverse * (gamma * gradient - normed * centre)).astype(bf16)
        low, high = made[:, :half], made[:, half:]
        keep_ref[at, :] = jnp.where(first, low, high)
        send_ref[at, :] = jnp.where(first, high, low)
        return gain

    gain = jnp.zeros((8, features), f32)
    scales.wait()
    for n in range(chunks):
        for copy in incoming[n]:
            copy.wait()
        gain = lax.fori_loop(n * height // step, (n + 1) * height // step, body, gain, unroll=3)
    gain_ref[...] = jnp.sum(gain, axis=0, keepdims=True)
    carried.wait()


def whole_kernel(core_ref, keep_ref, send_ref, grad_ref):
    half = keep_ref.shape[1]
    first = core_ref[0] == 0
    keep, send = keep_ref[...], send_ref[...]
    grad_ref[:, :half] = jnp.where(first, keep, send)
    grad_ref[:, half:] = jnp.where(first, send, keep)


def gain_tiles(gain_rows, gain, out_ref):
    rows = out_ref.shape[1] - 8
    for b, numbers in enumerate(gain_rows):
        if any(n is not None for n in numbers):
            lines = [
                jnp.zeros((1, LANES), f32) if n is None else gain[:, n * LANES:(n + 1) * LANES] for n in numbers
            ]
            lines += [jnp.zeros((1, LANES), f32)] * (8 - len(lines))
            out_ref[b, rows:, :LANES] = jnp.concatenate(lines, axis=0).astype(bf16)


def own_kernel(left_ref, right_ref, far_ref, out_ref, pair_ref, sem):
    carried = pltpu.make_async_copy(far_ref, pair_ref, sem)
    carried.start()
    out_ref[...] = jnp.dot(left_ref[...], right_ref[...], preferred_element_type=f32)
    carried.wait()


def weight_kernel(gain_rows, core_ref, own_ref, left_pair_ref, right_pair_ref, gain_ref, out_ref):
    blocks, height, width = out_ref.shape
    rows = height - 8
    gain = gain_ref[...]
    for b in range(blocks):
        at = slice(b * rows, (b + 1) * rows)
        out_ref[b, :rows, :] = (
            own_ref[at, :]
            + jnp.dot(left_pair_ref[at, :], right_pair_ref[...], preferred_element_type=f32)
        ).astype(bf16)
        out_ref[b, rows:, :] = jnp.zeros((8, width), bf16)
    for core, numbers in enumerate(gain_rows):
        pl.when(core_ref[0] == core)(functools.partial(gain_tiles, numbers, gain, out_ref))


def first_sum_kernel(middle, in_ref, out_ref):
    pieces, height, width = out_ref.shape
    pieces //= middle
    rows = (in_ref.shape[1] - 8) // middle
    total = in_ref[...].astype(f32).sum(0)
    for m in range(middle):
        for p in range(pieces):
            if p * height < rows:
                piece = total[m * rows + p * height:m * rows + (p + 1) * height, :]
            elif p * height == rows:
                piece = jnp.where(iota((height, width), 0) == 0, total[middle * rows + m:middle * rows + m + 1, :], 0.0)
            else:
                piece = jnp.zeros((height, width), f32)
            out_ref[m * pieces + p] = piece.astype(bf16)


def second_sum_kernel(in_ref, out_ref):
    total = in_ref[...].astype(f32).sum(0)
    total = total.astype(bf16)
    for b in range(out_ref.shape[0]):
        out_ref[b] = total


def joined_kernel(in_ref, weight_ref, note_ref):
    pieces, height, half = in_ref.shape
    part = weight_ref.shape[0] // 2
    squares = jnp.zeros((height, half), f32)
    gain = jnp.zeros((1, LANES), f32)
    for p in range(pieces):
        core = p % 2
        far, near = divmod((p // 2 - core) % (pieces // 2), 2)
        block = in_ref[p].astype(f32)
        if far * height < part:
            at = near * part + far * height
            squares += block * block
            weight_ref[at:at + height, core * half:(core + 1) * half] = block
        elif near == 0:
            gain += block[:1, :LANES]
    line = jnp.concatenate([gain, jnp.full((1, LANES), jnp.sum(squares), f32)], axis=1)
    for d in range(note_ref.shape[0]):
        note_ref[d] = line


def scale_kernel(features, note_ref, weight_ref, weight_out_ref, gain_out_ref):
    chunks = features // LANES
    notes = note_ref[...]
    squares = jnp.sum(jnp.max(notes[:, :, LANES:], axis=2))
    gain = notes[:chunks, :, :LANES]
    total = squares + jnp.sum(gain * gain)
    factor = f32(features) * lax.rsqrt(jnp.full((1, LANES), total + epsilon, f32))
    for n in range(chunks):
        gain_out_ref[n * LANES:(n + 1) * LANES] = (gain[n] * factor)[0]
        at = slice(n * LANES, (n + 1) * LANES)
        weight_out_ref[:, at] = weight_ref[:, at] * factor


def on_device(grad_rows, row_owner, acts, xact, gamma, w_out):
    seq_count = lax.axis_size(SEQ)
    counts = tuple(lax.axis_size(a) for a in (*DP, SEQ[0]))
    cells = [Cells(counts, core) for core in range(2)]
    inside = [group for c in cells for group in c.inside()]
    across = [group for c in cells for group in c.across()]
    tokens = row_owner.shape[1]
    slot_count, patches, features = acts.shape[2:]
    capacity = slot_count // seq_count
    rows = slot_count * patches
    half = features // 2
    core = jnp.reshape(lax.axis_index("core"), (1,)).astype(jnp.int32)
    swap = [(0, 1), (1, 0)]

    def shaped(dtype, *shape):
        return jax.ShapeDtypeStruct(shape, dtype)

    chunks = 3
    (outgoing,) = call(
        functools.partial(gather_kernel, seq_count, capacity, patches, chunks),
        "gather_rows",
        (shaped(bf16, rows, features),),
        (row_owner.reshape(1, tokens), grad_rows.reshape(tokens, patches, features)),
        far_out=(0,),
        limit=60,
        scratch=[pltpu.VMEM((rows, features), bf16), pltpu.SemaphoreType.DMA((chunks,))],
    )
    received = exchange(outgoing.reshape(seq_count, capacity * patches, features), SEQ)

    act_slots = acts.reshape(slot_count, patches, features)
    act_pair = lax.ppermute(act_slots, "core", swap)
    lines, inverse, left, left_pair = call(
        functools.partial(prepare_kernel, 8, [c.order() for c in cells]),
        "prepare",
        (
            shaped(bf16, rows, features),
            shaped(f32, rows, 1),
            shaped(bf16, features, rows),
            shaped(bf16, features, rows),
        ),
        (core, xact.reshape(slot_count, patches, features), act_slots, act_pair),
    )

    chunks = 8
    grad_keep, grad_send, left, gain_part = call(
        functools.partial(norm_kernel, chunks, 16),
        "norm_backward",
        (
            shaped(bf16, rows, half),
            shaped(bf16, rows, half),
            shaped(bf16, features, rows),
            shaped(f32, 1, features),
        ),
        (core, received.reshape(rows, features), lines, left, inverse, gamma.reshape(1, features)),
        far_in=(1, 2, 3, 4),
        limit=51.5,
        scratch=[
            pltpu.VMEM((rows, features), bf16),
            pltpu.VMEM((rows, features), bf16),
            pltpu.VMEM((rows, 1), f32),
            pltpu.SemaphoreType.DMA((2 * chunks,)),
            pltpu.SemaphoreType.DMA((2,)),
        ],
    )
    grad_pair = lax.ppermute(grad_send, "core", swap)
    (grad,) = call(
        whole_kernel, "whole_grad", (shaped(bf16, rows, features),), (core, grad_keep, grad_send), limit=52
    )
    own, left_pair = call(
        own_kernel,
        "weight_own",
        (shaped(f32, features, half), shaped(bf16, features, rows)),
        (left, grad_keep, left_pair),
        flops=2 * features * half * rows,
        far_in=(2,),
        limit=44,
        scratch=[pltpu.SemaphoreType.DMA],
    )
    grad, own = lax.optimization_barrier((grad, own))

    replicas = counts[0] * counts[1]
    out_rows = features // replicas
    z_rows = out_rows // 2 // (counts[2] // 2 - 1)
    (weight_pair,) = call(
        functools.partial(weight_kernel, [c.gain_rows(features // LANES) for c in cells]),
        "weight_pair",
        (shaped(bf16, 8, features // 8 + 8, half),),
        (core, own, left_pair, grad_pair, gain_part),
        flops=4 * features * half * rows,
    )
    (weight_some,) = call(
        functools.partial(first_sum_kernel, replicas // 4),
        "sum_first",
        (shaped(bf16, replicas // 4 * counts[2] // 2, z_rows, half),),
        (exchange(weight_pair, ALL, inside),),
    )
    (pieces,) = call(
        second_sum_kernel,
        "sum_second",
        (shaped(bf16, seq_count, z_rows, half),),
        (exchange(weight_some, ALL, across),),
    )
    weight_sum, note = call(
        joined_kernel,
        "joined",
        (shaped(f32, out_rows, features), shaped(f32, replicas, 1, 2 * LANES)),
        (exchange(pieces, SEQ),),
    )
    attn_grad = lax.dot_general(
        grad, w_out, (((1,), (1,)), ((), ())), preferred_element_type=f32
    ).astype(bf16).reshape(acts.shape)
    weight_grad, gain_grad = call(
        functools.partial(scale_kernel, features),
        "scaled",
        (shaped(f32, out_rows, features), shaped(f32, features)),
        (exchange(note, DP), weight_sum),
    )
    return (attn_grad, weight_grad, gain_grad)


def solution(mesh):
    finer = Mesh(mesh.devices.reshape(4, 8, mesh.shape["seq"] // 2, 2), ALL)
    placed = (
        P(DP, SEQ, None, None),
        P(DP, SEQ, None),
        P(DP, SEQ, None, None, None),
        P(DP, SEQ, None, None, None),
        P(),
        P(),
    )
    return jax.shard_map(
        on_device,
        mesh=finer,
        in_specs=placed,
        out_specs=(P(DP, SEQ, None, None, None), P(DP, None), P()),
        check_vma=False,
    )
```
